512 devices in a mesh: grp: 2 (over y), user: 64 (over z, core), head: 4 (over x).
Axes of the slice: x: 4, y: 2, z: 32, core: 2. Of those that a mesh axis runs over, the one named last changes fastest.
The devices are a block of a 4x8x32 slice.
Arguments:
- cand_ids: int32 [128, 512], P(('grp', 'user')), parts along dimension 0, may hold values from 0 to 32767, as said below
- prefix_len: int32 [128], P(('grp', 'user')), parts along dimension 0, may hold values from 1 to 512
- key_cache: bfloat16 [128, 512, 1024], P(('grp', 'user'), None, 'head'), parts along dimension 0, may hold values from -6 to 6
- value_cache: bfloat16 [128, 512, 1024], P(('grp', 'user'), None, 'head'), parts along dimension 0, may hold values from -6 to 6
- item_table: bfloat16 [32768, 1024], P('user'), may hold values from -6 to 6
- w_qkvu: bfloat16 [1024, 8, 4, 128], P(None, 'head'), may hold values from -0.1875 to 0.1875
- w_out: bfloat16 [8, 128, 1024], P('head'), may hold values from -0.1875 to 0.1875
Outputs:
- scores: float32 [128, 512], P(('grp', 'user')), parts along dimension 0
The draws below stay inside these ranges and needn't reach their ends.
There are 2 independent parts, one for each index of `grp`. The reference program is written for one: setup_inputs(seed, part) draws one part's arguments, and reference() takes and returns one part's arrays. A program takes and returns all parts, laid end to end along the dimension named above; an argument that names none is the same for every part. Nothing has to cross between parts.
Inputs may be any that keep to these rules, and one draw needn't show every extreme that they name: `cand_ids`: item id s * 512 + r lies in table shard s. Among the 512 candidates of each aligned block of 1 users, at most 16 lie in one table shard, and in every block some shard holds exactly 16 of them.
All inputs are finite; a program needn't handle non-finite values.
Results may differ from the reference program's by a relative error of at most 0.0095.
Values may be sent and summed in bfloat16 or wider, within the bound.
A program may use at most 64 MiB of HBM per device.

```python
import jax
import jax.numpy as jnp
from jax import lax

D = 1024
HEADS = 8
HD = 128
USR_DEV = 1
CAND = 512
PREF = 512
ROWS_SHARD = 512
USERS = 64
ITEMS = 32768
N_USER = 64
N_HEAD = 4


def draw_block(key):
    key_full, key_perm, key_shuffle, key_offset = jax.random.split(key, 4)
    row_count = USR_DEV * CAND
    capacity = 2 * row_count // N_USER
    slot_count = N_USER * capacity
    shard_ids = jnp.arange(slot_count, dtype=jnp.int32) // capacity
    full_shard = jax.random.randint(key_full, (), 0, N_USER, dtype=jnp.int32)
    permuted = jax.random.permutation(key_perm, slot_count).astype(jnp.int32)
    priority = permuted + jnp.where(shard_ids == full_shard, slot_count, 0).astype(jnp.int32)
    ordering = jnp.argsort(-priority, stable=True)
    chosen = shard_ids[ordering[:row_count]]
    chosen = jax.random.permutation(key_shuffle, chosen)
    offsets = jax.random.randint(key_offset, (row_count,), 0, ROWS_SHARD, dtype=jnp.int32)
    return (chosen * ROWS_SHARD + offsets).astype(jnp.int32)


def draw_cand_ids(key, part):
    block_keys = jax.random.split(jax.random.fold_in(key, 71), N_USER)
    blocks = jax.vmap(draw_block)(block_keys)
    return blocks.reshape(USR_DEV * N_USER, CAND).astype(jnp.int32)


def set_ends(entries, own_key, low, largest):
    spot = [jax.random.randint(jax.random.fold_in(own_key, axis), (), 0, length) for axis, length in enumerate(entries.shape)]
    widest = entries.shape.index(max(entries.shape))
    neighbour = spot[:widest] + [(spot[widest] + 1) % entries.shape[widest]] + spot[widest + 1:]
    return entries.at[tuple(spot)].set(low).at[tuple(neighbour)].set(largest)


def level_of(stream_key, extent, shards, low, largest):
    def one(position, parts):
        heights = jax.random.uniform(jax.random.fold_in(jax.random.fold_in(stream_key, 6), position), (parts,), jnp.float32, low / len(shards), largest / len(shards))
        return jnp.repeat(jnp.exp(heights), extent[position] // parts).reshape((-1,) + (1,) * (len(extent) - position - 1))

    factor_of = one(*shards[0])
    for cut in shards[1:]:
        factor_of = factor_of * one(*cut)
    return factor_of


def bell_draw(rng, dims, deviation, limit, cuts=(), held_as=jnp.bfloat16):
    entries = jax.random.normal(rng, dims, jnp.float32) * deviation
    if len(cuts) > 0:
        entries = level_of(rng, dims, cuts, -0.22, 0.18) * entries
    return jnp.clip(entries, min=-limit, max=limit).astype(held_as)


def setup_inputs(seed: int = 0, part: int = 0) -> dict:
    keys = jax.random.split(jax.random.key(seed), 8)
    part_keys = jax.random.split(jax.random.fold_in(keys[7], part), 8)
    cand_ids = draw_cand_ids(jax.random.fold_in(jax.random.fold_in(keys[7], part), 71), part)
    prefix_len = set_ends(jax.random.randint(part_keys[1], (USERS,), 1, PREF + 1), jax.random.fold_in(part_keys[1], 1), 1, PREF).astype(jnp.int32)
    key_cache = bell_draw(part_keys[2], (USERS, PREF, D), 1.0, 6.0, ((0, 64), (2, 4)))
    value_cache = bell_draw(part_keys[3], (USERS, PREF, D), 1.0, 6.0, ((0, 64), (2, 4)))
    item_table = bell_draw(keys[4], (ITEMS, D), 1.0, 6.0, ((0, 64),))
    w_qkvu = bell_draw(keys[5], (D, HEADS, 4, HD), D ** -0.5, 0.1875, ((1, 4),))
    w_out = bell_draw(keys[6], (HEADS, HD, D), D ** -0.5, 0.1875, ((0, 4),))
    return {"cand_ids": cand_ids, "prefix_len": prefix_len, "key_cache": key_cache, "value_cache": value_cache, "item_table": item_table, "w_qkvu": w_qkvu, "w_out": w_out}


def reference(cand_ids, prefix_len, key_cache, value_cache, item_table, w_qkvu, w_out):
    score_scale = HD ** (-0.5)
    flat_weight = w_qkvu.reshape(D, HEADS * 4 * HD)
    group_width = HEADS // N_HEAD * HD
    w_groups = w_out.reshape(N_HEAD, group_width, D).astype(jnp.float32)

    def one_user(packed):
        item_ids, length, cached_keys, cached_values = packed
        embedded = item_table[item_ids.astype(jnp.int32)]
        projected = jnp.dot(embedded, flat_weight, preferred_element_type=jnp.float32)
        activated = jax.nn.silu(projected).astype(jnp.bfloat16).reshape(CAND, HEADS, 4, HD)
        queries = activated[:, :, 0].astype(jnp.float32)
        own_keys = activated[:, :, 1].astype(jnp.float32)
        own_values = activated[:, :, 2].astype(jnp.float32)
        gates = activated[:, :, 3].astype(jnp.float32)
        keys_all = cached_keys.reshape(PREF, HEADS, HD).astype(jnp.float32)
        values_all = cached_values.reshape(PREF, HEADS, HD).astype(jnp.float32)
        raw = jnp.einsum('chd,phd->hcp', queries, keys_all)
        denominator = (length + 1).astype(jnp.float32)
        in_prefix = jnp.arange(PREF, dtype=jnp.int32) < length
        weights = jnp.where(in_prefix[None, None, :], jax.nn.silu(raw * score_scale), 0.0) / denominator
        weights = weights.astype(jnp.bfloat16).astype(jnp.float32)
        attended = jnp.einsum('hcp,phd->chd', weights, values_all)
        own_weight = jax.nn.silu(lax.optimization_barrier(jnp.sum(queries * own_keys, axis=-1)) * score_scale) / denominator
        attended = attended + own_weight[:, :, None] * own_values
        mean_square = lax.optimization_barrier(jnp.mean(attended * attended, axis=-1, keepdims=True))
        gated = (attended * lax.rsqrt(mean_square + 1e-06) * gates).astype(jnp.bfloat16)
        group_rows = gated.reshape(CAND, N_HEAD, group_width).astype(jnp.float32)
        partial_value = jnp.einsum('cgk,gkd->gcd', group_rows, w_groups).astype(jnp.bfloat16)
        summed = lax.optimization_barrier(jnp.sum(partial_value.astype(jnp.float32), axis=0))
        inner = lax.optimization_barrier(jnp.sum(summed * embedded.astype(jnp.float32), axis=-1)) * D ** (-0.5)
        return inner * lax.rsqrt(lax.optimization_barrier(jnp.mean(summed * summed, axis=-1)) + 1e-06)
    return lax.map(one_user, (cand_ids, prefix_len, key_cache, value_cache))
```

```python
import functools

import jax
import jax.numpy as jnp
from jax import lax
from jax.experimental import pallas as pl
from jax.experimental.pallas import tpu as pltpu
from jax.sharding import PartitionSpec as P

MESH = pl.DeviceIdType.MESH
NT = (((1,), (1,)), ((), ()))
TN = (((0,), (0,)), ((), ()))


def log2(n):
    assert n & (n - 1) == 0
    return n.bit_length() - 1


def silu(v):
    half = 0.5 * v
    return half + half * jnp.tanh(half)


def kernel(
    nz, nh, cap, ids_ref, len_ref, k_hbm, v_hbm, table_hbm, wq_hbm, wo_hbm, out_ref,
    table, wq, keys, values, wfull, req, req_in, rows, emb, gout, gat, slots, part, parts,
    load_sem, req_send, req_recv, row_send, row_recv, fwd_send, fwd_recv, gat_send, gat_recv,
    w_send, w_recv, wp_send, wp_recv, s_send, s_recv,
):
    f32, bf16, i32 = jnp.float32, jnp.bfloat16, jnp.int32
    u, x = lax.axis_index("user"), lax.axis_index("head")
    z, c = u // 2, u % 2
    steps = nz // nh
    n = ids_ref.shape[1]
    shard_rows, d_model = table.shape
    blocks = 2 * nh * steps
    own_class = x + c * (1 - 2 * (x % 2))

    def offset(quarter, j):
        half, odd = j // 2, j % 2
        return quarter + nh * (half + odd * (steps - 1 - 2 * half))

    def shard(j, core):
        quarter = x if core == 0 else x + 1 - 2 * (x % 2)
        return 2 * ((z + offset(quarter, j)) % nz) + core

    def requester(j, core):
        return 2 * ((z + nz - offset(own_class, j)) % nz) + core

    def head(d):
        return (x + d) % nh

    partner = u + 1 - 2 * c

    barrier = pltpu.get_barrier_semaphore()

    def greet(j, carry):
        for core in (0, 1):
            for user in (shard(j, core), requester(j, core)):

                @pl.when(user != u)
                def _():
                    pl.semaphore_signal(
                        barrier, inc=1, device_id={"user": user}, device_id_type=MESH
                    )

        return carry

    lax.fori_loop(0, steps, greet, 0)
    for d in range(1, nh):
        pl.semaphore_signal(barrier, inc=1, device_id={"head": head(d)}, device_id_type=MESH)
    pl.semaphore_signal(barrier, inc=1, device_id={"user": partner}, device_id_type=MESH)

    loads = [
        pltpu.make_async_copy(src, dst, load_sem.at[i])
        for i, (src, dst) in enumerate(
            (
                (table_hbm, table),
                (wq_hbm, wq),
                (k_hbm.at[0], keys),
                (v_hbm.at[0], values),
                (wo_hbm, wfull.at[x]),
            )
        )
    ]
    for load in loads:
        load.start()

    ids = ids_ref[...]
    shard_of = ids >> log2(shard_rows)
    local = ids & (shard_rows - 1)
    core_of = shard_of & 1
    off = ((shard_of >> 1) - z) & (nz - 1)
    turn = off >> log2(nh)
    owner = (off & (nh - 1)) ^ core_of
    step_of = jnp.where(turn < steps // 2, 2 * turn, 2 * (steps - 1 - turn) + 1)
    block_of = (step_of * nh + owner) * 2 + core_of
    in_block = lax.broadcasted_iota(i32, (blocks, n), 0) == block_of
    one_hot = jnp.where(in_block, 1.0, 0.0).astype(bf16)
    before = lax.broadcasted_iota(i32, (n, n), 0) < lax.broadcasted_iota(i32, (n, n), 1)
    earlier = jnp.dot(
        one_hot, jnp.where(before, 1.0, 0.0).astype(bf16), preferred_element_type=f32
    )
    place = jnp.sum(jnp.where(in_block, earlier, 0.0), axis=0, keepdims=True).astype(i32)
    slots[...] = block_of * cap + place
    at_place = (lax.broadcasted_iota(i32, (128, n), 0) & (cap - 1)) == place
    high = jnp.where(at_place, (local >> 5).astype(f32), 0.0).astype(bf16)
    low = jnp.where(at_place, (local & 31).astype(f32), 0.0).astype(bf16)
    wanted = (
        lax.dot_general(one_hot, high, NT, preferred_element_type=f32) * 32.0
        + lax.dot_general(one_hot, low, NT, preferred_element_type=f32)
    ).astype(i32)
    for b in range(blocks):
        req[b] = wanted[b : b + 1]

    others = (own_class + nh - 1) // nh
    pl.semaphore_wait(barrier, 4 * steps + nh - 2 + 2 * others)

    def to_user(src, dst, send_sem, recv_sem, user):
        return pltpu.make_async_remote_copy(
            src_ref=src,
            dst_ref=dst,
            send_sem=send_sem,
            recv_sem=recv_sem,
            device_id={"user": user},
            device_id_type=MESH,
        )

    def to_head(src, dst, send_sem, recv_sem, d):
        return pltpu.make_async_remote_copy(
            src_ref=src,
            dst_ref=dst,
            send_sem=send_sem,
            recv_sem=recv_sem,
            device_id={"head": head(d)},
            device_id_type=MESH,
        )

    def start_unless_self(copy, src, dst, recv_sem, user):
        @pl.when(user != u)
        def _():
            copy.start()

        @pl.when(user == u)
        def _():
            pltpu.make_async_copy(src, dst, recv_sem).start()

    def request(j, core):
        user = shard(j, core)
        src, dst = req.at[(j * nh + x) * 2 + core], req_in.at[j, c]
        return to_user(src, dst, req_send.at[j, core], req_recv.at[j], user), src, dst, user

    def ask(j, carry):
        for core in (0, 1):
            copy, src, dst, user = request(j, core)
            start_unless_self(copy, src, dst, req_recv.at[j], user)
        return carry

    lax.fori_loop(0, steps, ask, 0)

    def half_out(d):
        return to_head(wo_hbm.at[c], wfull.at[x, c], w_send.at[d - 1], w_recv.at[d - 1], d)

    for d in range(1, nh):
        half_out(d).start()

    loads[0].wait()

    def answer(j, core):
        user = requester(j, core)
        src, dst = rows.at[j, core], emb.at[j, x, c]
        return to_user(src, dst, row_send.at[j, core], row_recv.at[j], user), src, dst, user

    def serve(j, carry):
        pltpu.make_async_copy(req_in.at[j], req_in.at[j], req_recv.at[j]).wait()
        lane = lax.broadcasted_iota(i32, (1, 2 * cap), 1)
        both = jnp.where(lane < cap, req_in[j, 0][:, : 2 * cap], req_in[j, 1][:, : 2 * cap])
        pick = lax.broadcasted_iota(i32, (shard_rows, 2 * cap), 0) == both
        found = lax.dot_general(
            jnp.where(pick, 1.0, 0.0).astype(bf16), table[...], TN, preferred_element_type=f32
        )
        rows[j] = found.astype(bf16).reshape(2, cap, d_model)
        for core in (0, 1):
            copy, src, dst, user = answer(j, core)
            start_unless_self(copy, src, dst, row_recv.at[j], user)
        return carry

    lax.fori_loop(0, steps, serve, 0)

    def half_on(d):
        piece = wfull.at[(x + nh - d) % nh, c]
        return to_user(piece, piece, wp_send.at[d - 1], wp_recv.at[d - 1], partner)

    for d in range(1, nh):
        piece = wfull.at[(x + nh - d) % nh, c]
        pltpu.make_async_copy(piece, piece, w_recv.at[d - 1]).wait()
        half_on(d).start()

    for load in loads[1:]:
        load.wait()

    length = len_ref[0, 0]
    head_size = 128
    heads_here = keys.shape[1] // head_size
    prefix = keys.shape[0]
    scale = head_size ** (-0.5)
    per_token = 1.0 / (jnp.zeros((1, 1), f32) + (length + 1).astype(f32))
    inside = lax.broadcasted_iota(i32, (1, prefix), 1) < length
    factor = jnp.where(inside, (0.5 * scale) * per_token, 0.0)

    def forward(j, d):
        mine = emb.at[j, x]
        return to_head(mine, mine, fwd_send.at[j, d - 1], fwd_recv.at[j, d - 1], d)

    def give(j, d):
        return to_head(
            gout.at[j, head(d)], gat.at[j, x], gat_send.at[j, d - 1], gat_recv.at[j, d - 1], d
        )

    def compute(j):
        for d in range(1, nh):
            theirs = emb.at[j, (x + nh - d) % nh]
            pltpu.make_async_copy(theirs, theirs, fwd_recv.at[j, d - 1]).wait()
        embedded = emb[j].reshape(nh * 2 * cap, d_model)
        projected = jnp.dot(embedded, wq[...], preferred_element_type=f32)
        activated = silu(projected).astype(bf16)
        for h in range(heads_here):
            columns = slice(h * head_size, (h + 1) * head_size)
            queries, own_keys, own_values, gates = (
                activated[:, (4 * h + i) * head_size : (4 * h + i + 1) * head_size]
                for i in range(4)
            )
            raw = lax.dot_general(queries, keys[:, columns], NT, preferred_element_type=f32)
            weights = (raw * factor) * (1.0 + jnp.tanh(raw * (0.5 * scale)))
            attended = jnp.dot(
                weights.astype(bf16), values[:, columns], preferred_element_type=f32
            )
            own_dot = jnp.sum(
                queries.astype(f32) * own_keys.astype(f32), axis=1, keepdims=True
            )
            own_weight = silu(own_dot * scale) * per_token
            attended = attended + own_weight * own_values.astype(f32)
            mean_square = jnp.mean(attended * attended, axis=1, keepdims=True)
            gated = attended * lax.rsqrt(mean_square + 1e-06) * gates.astype(f32)
            gout[j, :, :, columns] = gated.astype(bf16).reshape(nh, 2 * cap, head_size)
        for d in range(1, nh):
            give(j, d).start()

    def stage(j, carry):
        @pl.when(j < steps)
        def _():
            mine = emb.at[j, x]
            pltpu.make_async_copy(mine, mine, row_recv.at[j]).wait()
            for d in range(1, nh):
                forward(j, d).start()

        @pl.when(j >= 1)
        def _():
            compute(j - 1)

        return carry

    lax.fori_loop(0, steps + 1, stage, 0)

    for d in range(1, nh):
        piece = wfull.at[(x + nh - d) % nh, 1 - c]
        pltpu.make_async_copy(piece, piece, wp_recv.at[d - 1]).wait()

    def collect(j, carry):
        for d in range(1, nh):
            theirs = gat.at[j, (x + nh - d) % nh]
            pltpu.make_async_copy(theirs, theirs, gat_recv.at[j, d - 1]).wait()
        gat[j, x] = gout[j, x]
        return carry

    lax.fori_loop(0, steps, collect, 0)
    own = steps * 2 * cap
    width = gat.shape[-1]
    summed = jnp.zeros((own, d_model), f32)
    for y in range(nh):
        summed = summed + jnp.dot(
            gat[:, y].reshape(own, width),
            wfull[y].reshape(width, d_model),
            preferred_element_type=f32,
        )
    mine = emb[:, pl.ds(x, 1)].reshape(own, d_model).astype(f32)
    inner = jnp.sum(summed * mine, axis=1, keepdims=True)
    square = jnp.sum(summed * summed, axis=1, keepdims=True)
    score = inner * d_model ** (-0.5) * lax.rsqrt(square / d_model + 1e-06)
    row = lax.broadcasted_iota(i32, (own, n), 0)
    slot = ((row >> log2(2 * cap)) * nh + x) * (2 * cap) + (row & (2 * cap - 1))
    part[...] = jnp.sum(jnp.where(slot == slots[...], score, 0.0), axis=0, keepdims=True)

    def share(d):
        return to_head(part, parts.at[d - 1], s_send.at[d - 1], s_recv.at[d - 1], d)

    for d in range(1, nh):
        share(d).start()
    total = part[...]
    for d in range(1, nh):
        pltpu.make_async_copy(parts.at[d - 1], parts.at[d - 1], s_recv.at[d - 1]).wait()
        total = total + parts[d - 1]
    out_ref[...] = total

    def drain(j, carry):
        for core in (0, 1):
            for make in (request, answer):
                copy, _, _, user = make(j, core)

                @pl.when(user != u)
                def _():
                    copy.wait_send()

        for d in range(1, nh):
            forward(j, d).wait_send()
            give(j, d).wait_send()
        return carry

    lax.fori_loop(0, steps, drain, 0)
    for d in range(1, nh):
        half_out(d).wait_send()
        half_on(d).wait_send()
        share(d).wait_send()


def body(nz, nh, cand_ids, prefix_len, key_cache, value_cache, item_table, w_qkvu, w_out):
    n = cand_ids.shape[1]
    prefix, width = key_cache.shape[1:]
    shard_rows, d_model = item_table.shape
    steps = nz // nh
    blocks = 2 * nz
    cap = 2 * n // blocks
    bf16, dma = jnp.bfloat16, pltpu.SemaphoreType.DMA
    vmem = pl.BlockSpec(memory_space=pltpu.VMEM)
    hbm = pl.BlockSpec(memory_space=pl.ANY)
    wq = w_qkvu.reshape(d_model, -1)
    return pl.pallas_call(
        functools.partial(kernel, nz, nh, cap),
        out_shape=jax.ShapeDtypeStruct((1, n), jnp.float32),
        in_specs=[vmem, pl.BlockSpec(memory_space=pltpu.SMEM)] + [hbm] * 5,
        out_specs=vmem,
        scratch_shapes=[
            pltpu.VMEM((shard_rows, d_model), bf16),
            pltpu.VMEM(wq.shape, bf16),
            pltpu.VMEM((prefix, width), bf16),
            pltpu.VMEM((prefix, width), bf16),
            pltpu.VMEM((nh, *w_out.shape), bf16),
            pltpu.VMEM((blocks, 1, 128), jnp.int32),
            pltpu.VMEM((steps, 2, 1, 128), jnp.int32),
            pltpu.VMEM((steps, 2, cap, d_model), bf16),
            pltpu.VMEM((steps, nh, 2, cap, d_model), bf16),
            pltpu.VMEM((steps, nh, 2 * cap, width), bf16),
            pltpu.VMEM((steps, nh, 2 * cap, width), bf16),
            pltpu.VMEM((1, n), jnp.int32),
            pltpu.VMEM((1, n), jnp.float32),
            pltpu.VMEM((nh - 1, 1, n), jnp.float32),
            dma((5,)),
            dma((steps, 2)),
            dma((steps,)),
            dma((steps, 2)),
            dma((steps,)),
            dma((steps, nh - 1)),
            dma((steps, nh - 1)),
            dma((steps, nh - 1)),
            dma((steps, nh - 1)),
            dma((nh - 1,)),
            dma((nh - 1,)),
            dma((nh - 1,)),
            dma((nh - 1,)),
            dma((nh - 1,)),
            dma((nh - 1,)),
        ],
        compiler_params=pltpu.CompilerParams(
            collective_id=0, has_side_effects=True, vmem_limit_bytes=48 * 1024 * 1024
        ),
    )(cand_ids, prefix_len.reshape(1, 1), key_cache, value_cache, item_table, wq, w_out)


def solution(mesh):
    users = ("grp", "user")
    return jax.shard_map(
        functools.partial(body, mesh.shape["user"] // 2, mesh.shape["head"]),
        mesh=mesh,
        in_specs=(
            P(users, None),
            P(users),
            P(users, None, "head"),
            P(users, None, "head"),
            P("user", None),
            P(None, "head", None, None),
            P("head", None, None),
        ),
        out_specs=P(users, None),
        check_vma=False,
    )
```

```python
import functools

import jax
import jax.numpy as jnp
from jax import lax
from jax.experimental import pallas as pl
from jax.experimental.pallas import tpu as pltpu
from jax.sharding import PartitionSpec as P

MESH = pl.DeviceIdType.MESH
NT = (((1,), (1,)), ((), ()))
TN = (((0,), (0,)), ((), ()))


def log2(n):
    assert n & (n - 1) == 0
    return n.bit_length() - 1


def silu(v):
    half = 0.5 * v
    return half + half * jnp.tanh(half)


def kernel(
    nz, nh, cap, ids_ref, len_ref, k_hbm, v_hbm, table_hbm, wq_hbm, wo_hbm, out_ref,
    table, wq_in, wq, keys, values, wfull, req, req_in, rows, emb, gout, gat, slots, part, parts,
    load_sem, req_send, req_recv, row_send, row_recv, fwd_send, fwd_recv, gat_send, gat_recv,
    w_send, w_recv, wp_send, wp_recv, s_send, s_recv,
):
    f32, bf16, i32 = jnp.float32, jnp.bfloat16, jnp.int32
    u, x = lax.axis_index("user"), lax.axis_index("head")
    z, c = u // 2, u % 2
    steps = nz // nh
    n = ids_ref.shape[1]
    shard_rows, d_model = table.shape
    blocks = 2 * nh * steps
    own_class = x + c * (1 - 2 * (x % 2))

    def offset(quarter, j):
        half, odd = j // 2, j % 2
        return quarter + nh * (half + odd * (steps - 1 - 2 * half))

    def shard(j, core):
        quarter = x if core == 0 else x + 1 - 2 * (x % 2)
        return 2 * ((z + offset(quarter, j)) % nz) + core

    def requester(j, core):
        return 2 * ((z + nz - offset(own_class, j)) % nz) + core

    def head(d):
        return (x + d) % nh

    partner = u + 1 - 2 * c

    barrier = pltpu.get_barrier_semaphore()

    def greet(j, carry):
        for core in (0, 1):
            for user in (shard(j, core), requester(j, core)):

                @pl.when(user != u)
                def _():
                    pl.semaphore_signal(
                        barrier, inc=1, device_id={"user": user}, device_id_type=MESH
                    )

        return carry

    lax.fori_loop(0, steps, greet, 0)
    for d in range(1, nh):
        pl.semaphore_signal(barrier, inc=1, device_id={"head": head(d)}, device_id_type=MESH)
    pl.semaphore_signal(barrier, inc=1, device_id={"user": partner}, device_id_type=MESH)

    loads = [
        pltpu.make_async_copy(src, dst, load_sem.at[i])
        for i, (src, dst) in enumerate(
            (
                (table_hbm, table),
                (wq_hbm, wq_in),
                (k_hbm.at[0], keys),
                (v_hbm.at[0], values),
                (wo_hbm, wfull.at[x]),
            )
        )
    ]
    for load in loads:
        load.start()

    ids = ids_ref[...]
    shard_of = ids >> log2(shard_rows)
    local = ids & (shard_rows - 1)
    core_of = shard_of & 1
    off = ((shard_of >> 1) - z) & (nz - 1)
    turn = off >> log2(nh)
    owner = (off & (nh - 1)) ^ core_of
    step_of = jnp.where(turn < steps // 2, 2 * turn, 2 * (steps - 1 - turn) + 1)
    block_of = (step_of * nh + owner) * 2 + core_of
    in_block = lax.broadcasted_iota(i32, (blocks, n), 0) == block_of
    one_hot = jnp.where(in_block, 1.0, 0.0).astype(bf16)
    before = lax.broadcasted_iota(i32, (n, n), 0) < lax.broadcasted_iota(i32, (n, n), 1)
    earlier = jnp.dot(
        one_hot, jnp.where(before, 1.0, 0.0).astype(bf16), preferred_element_type=f32
    )
    place = jnp.sum(jnp.where(in_block, earlier, 0.0), axis=0, keepdims=True).astype(i32)
    slots[...] = block_of * cap + place
    at_place = (lax.broadcasted_iota(i32, (128, n), 0) & (cap - 1)) == place
    high = jnp.where(at_place, (local >> 5).astype(f32), 0.0).astype(bf16)
    low = jnp.where(at_place, (local & 31).astype(f32), 0.0).astype(bf16)
    wanted = (
        lax.dot_general(one_hot, high, NT, preferred_element_type=f32) * 32.0
        + lax.dot_general(one_hot, low, NT, preferred_element_type=f32)
    ).astype(i32)
    for b in range(blocks):
        req[b] = wanted[b : b + 1]

    others = (own_class + nh - 1) // nh
    for load in loads[1:]:
        load.wait()
    span = 128

    def relay_weights(i, carry):
        at = pl.ds(pl.multiple_of(i * span, span), span)
        wq[at, :] = wq_in[at].reshape(span, wq.shape[1])
        return carry

    lax.fori_loop(0, d_model // span, relay_weights, 0)

    pl.semaphore_wait(barrier, 4 * steps + nh - 2 + 2 * others)

    def to_user(src, dst, send_sem, recv_sem, user):
        return pltpu.make_async_remote_copy(
            src_ref=src,
            dst_ref=dst,
            send_sem=send_sem,
            recv_sem=recv_sem,
            device_id={"user": user},
            device_id_type=MESH,
        )

    def to_head(src, dst, send_sem, recv_sem, d):
        return pltpu.make_async_remote_copy(
            src_ref=src,
            dst_ref=dst,
            send_sem=send_sem,
            recv_sem=recv_sem,
            device_id={"head": head(d)},
            device_id_type=MESH,
        )

    def start_unless_self(copy, src, dst, recv_sem, user):
        @pl.when(user != u)
        def _():
            copy.start()

        @pl.when(user == u)
        def _():
            pltpu.make_async_copy(src, dst, recv_sem).start()

    def request(j, core):
        user = shard(j, core)
        src, dst = req.at[(j * nh + x) * 2 + core], req_in.at[j, c]
        return to_user(src, dst, req_send.at[j, core], req_recv.at[j], user), src, dst, user

    def ask(j, carry):
        for core in (0, 1):
            copy, src, dst, user = request(j, core)
            start_unless_self(copy, src, dst, req_recv.at[j], user)
        return carry

    lax.fori_loop(0, steps, ask, 0)

    def half_out(d):
        return to_head(wo_hbm.at[c], wfull.at[x, c], w_send.at[d - 1], w_recv.at[d - 1], d)

    for d in range(1, nh):
        half_out(d).start()

    loads[0].wait()

    def answer(j, core):
        user = requester(j, core)
        src, dst = rows.at[j, core], emb.at[j, x, c]
        return to_user(src, dst, row_send.at[j, core], row_recv.at[j], user), src, dst, user

    def serve(j, carry):
        pltpu.make_async_copy(req_in.at[j], req_in.at[j], req_recv.at[j]).wait()
        lane = lax.broadcasted_iota(i32, (1, 2 * cap), 1)
        both = jnp.where(lane < cap, req_in[j, 0][:, : 2 * cap], req_in[j, 1][:, : 2 * cap])
        pick = lax.broadcasted_iota(i32, (shard_rows, 2 * cap), 0) == both
        found = lax.dot_general(
            jnp.where(pick, 1.0, 0.0).astype(bf16), table[...], TN, preferred_element_type=f32
        )
        rows[j] = found.astype(bf16).reshape(2, cap, d_model)
        for core in (0, 1):
            copy, src, dst, user = answer(j, core)
            start_unless_self(copy, src, dst, row_recv.at[j], user)
        return carry

    lax.fori_loop(0, steps, serve, 0)

    def half_on(d):
        piece = wfull.at[(x + nh - d) % nh, c]
        return to_user(piece, piece, wp_send.at[d - 1], wp_recv.at[d - 1], partner)

    for d in range(1, nh):
        piece = wfull.at[(x + nh - d) % nh, c]
        pltpu.make_async_copy(piece, piece, w_recv.at[d - 1]).wait()
        half_on(d).start()

    length = len_ref[0, 0]
    head_size = 128
    heads_here = keys.shape[1] // head_size
    prefix = keys.shape[0]
    scale = head_size ** (-0.5)
    per_token = 1.0 / (jnp.zeros((1, 1), f32) + (length + 1).astype(f32))
    inside = lax.broadcasted_iota(i32, (1, prefix), 1) < length
    factor = jnp.where(inside, (0.5 * scale) * per_token, 0.0)

    def forward(j, d):
        mine = emb.at[j, x]
        return to_head(mine, mine, fwd_send.at[j, d - 1], fwd_recv.at[j, d - 1], d)

    def give(j, d):
        return to_head(
            gout.at[j, head(d)], gat.at[j, x], gat_send.at[j, d - 1], gat_recv.at[j, d - 1], d
        )

    def compute(j):
        for d in range(1, nh):
            theirs = emb.at[j, (x + nh - d) % nh]
            pltpu.make_async_copy(theirs, theirs, fwd_recv.at[j, d - 1]).wait()
        embedded = emb[j].reshape(nh * 2 * cap, d_model)
        projected = jnp.dot(embedded, wq[...], preferred_element_type=f32)
        activated = silu(projected).astype(bf16)
        for h in range(heads_here):
            columns = slice(h * head_size, (h + 1) * head_size)
            queries, own_keys, own_values, gates = (
                activated[:, (4 * h + i) * head_size : (4 * h + i + 1) * head_size]
                for i in range(4)
            )
            raw = lax.dot_general(queries, keys[:, columns], NT, preferred_element_type=f32)
            weights = (raw * factor) * (1.0 + jnp.tanh(raw * (0.5 * scale)))
            attended = jnp.dot(
                weights.astype(bf16), values[:, columns], preferred_element_type=f32
            )
            own_dot = jnp.sum(
                queries.astype(f32) * own_keys.astype(f32), axis=1, keepdims=True
            )
            own_weight = silu(own_dot * scale) * per_token
            attended = attended + own_weight * own_values.astype(f32)
            mean_square = jnp.mean(attended * attended, axis=1, keepdims=True)
            gated = attended * lax.rsqrt(mean_square + 1e-06) * gates.astype(f32)
            gout[j, :, :, columns] = gated.astype(bf16).reshape(nh, 2 * cap, head_size)
        for d in range(1, nh):
            give(j, d).start()

    def stage(j, carry):
        @pl.when(j < steps)
        def _():
            mine = emb.at[j, x]
            pltpu.make_async_copy(mine, mine, row_recv.at[j]).wait()
            for d in range(1, nh):
                forward(j, d).start()

        @pl.when(j >= 1)
        def _():
            compute(j - 1)

        return carry

    lax.fori_loop(0, steps + 1, stage, 0)

    for d in range(1, nh):
        piece = wfull.at[(x + nh - d) % nh, 1 - c]
        pltpu.make_async_copy(piece, piece, wp_recv.at[d - 1]).wait()

    def collect(j, carry):
        for d in range(1, nh):
            theirs = gat.at[j, (x + nh - d) % nh]
            pltpu.make_async_copy(theirs, theirs, gat_recv.at[j, d - 1]).wait()
        gat[j, x] = gout[j, x]
        return carry

    lax.fori_loop(0, steps, collect, 0)
    own = steps * 2 * cap
    width = gat.shape[-1]
    summed = jnp.zeros((own, d_model), f32)
    for y in range(nh):
        summed = summed + jnp.dot(
            gat[:, y].reshape(own, width),
            wfull[y].reshape(width, d_model),
            preferred_element_type=f32,
        )
    mine = emb[:, pl.ds(x, 1)].reshape(own, d_model).astype(f32)
    inner = jnp.sum(summed * mine, axis=1, keepdims=True)
    square = jnp.sum(summed * summed, axis=1, keepdims=True)
    score = inner * d_model ** (-0.5) * lax.rsqrt(square / d_model + 1e-06)
    row = lax.broadcasted_iota(i32, (own, n), 0)
    slot = ((row >> log2(2 * cap)) * nh + x) * (2 * cap) + (row & (2 * cap - 1))
    part[...] = jnp.sum(jnp.where(slot == slots[...], score, 0.0), axis=0, keepdims=True)

    def share(d):
        return to_head(part, parts.at[d - 1], s_send.at[d - 1], s_recv.at[d - 1], d)

    for d in range(1, nh):
        share(d).start()
    total = part[...]
    for d in range(1, nh):
        pltpu.make_async_copy(parts.at[d - 1], parts.at[d - 1], s_recv.at[d - 1]).wait()
        total = total + parts[d - 1]
    out_ref[...] = total

    def drain(j, carry):
        for core in (0, 1):
            for make in (request, answer):
                copy, _, _, user = make(j, core)

                @pl.when(user != u)
                def _():
                    copy.wait_send()

        for d in range(1, nh):
            forward(j, d).wait_send()
            give(j, d).wait_send()
        return carry

    lax.fori_loop(0, steps, drain, 0)
    for d in range(1, nh):
        half_out(d).wait_send()
        half_on(d).wait_send()
        share(d).wait_send()


def body(nz, nh, cand_ids, prefix_len, key_cache, value_cache, item_table, w_qkvu, w_out):
    n = cand_ids.shape[1]
    prefix, width = key_cache.shape[1:]
    shard_rows, d_model = item_table.shape
    steps = nz // nh
    blocks = 2 * nz
    cap = 2 * n // blocks
    bf16, dma = jnp.bfloat16, pltpu.SemaphoreType.DMA
    vmem = pl.BlockSpec(memory_space=pltpu.VMEM)
    hbm = pl.BlockSpec(memory_space=pl.ANY)
    wq_width = w_qkvu.size // d_model
    return pl.pallas_call(
        functools.partial(kernel, nz, nh, cap),
        out_shape=jax.ShapeDtypeStruct((1, n), jnp.float32),
        in_specs=[vmem, pl.BlockSpec(memory_space=pltpu.SMEM)] + [hbm] * 5,
        out_specs=vmem,
        scratch_shapes=[
            pltpu.VMEM((shard_rows, d_model), bf16),
            pltpu.VMEM(w_qkvu.shape, bf16),
            pltpu.VMEM((d_model, wq_width), bf16),
            pltpu.VMEM((prefix, width), bf16),
            pltpu.VMEM((prefix, width), bf16),
            pltpu.VMEM((nh, *w_out.shape), bf16),
            pltpu.VMEM((blocks, 1, 128), jnp.int32),
            pltpu.VMEM((steps, 2, 1, 128), jnp.int32),
            pltpu.VMEM((steps, 2, cap, d_model), bf16),
            pltpu.VMEM((steps, nh, 2, cap, d_model), bf16),
            pltpu.VMEM((steps, nh, 2 * cap, width), bf16),
            pltpu.VMEM((steps, nh, 2 * cap, width), bf16),
            pltpu.VMEM((1, n), jnp.int32),
            pltpu.VMEM((1, n), jnp.float32),
            pltpu.VMEM((nh - 1, 1, n), jnp.float32),
            dma((5,)),
            dma((steps, 2)),
            dma((steps,)),
            dma((steps, 2)),
            dma((steps,)),
            dma((steps, nh - 1)),
            dma((steps, nh - 1)),
            dma((steps, nh - 1)),
            dma((steps, nh - 1)),
            dma((nh - 1,)),
            dma((nh - 1,)),
            dma((nh - 1,)),
            dma((nh - 1,)),
            dma((nh - 1,)),
            dma((nh - 1,)),
        ],
        compiler_params=pltpu.CompilerParams(
            collective_id=0, has_side_effects=True, vmem_limit_bytes=67_043_328
        ),
    )(cand_ids, prefix_len.reshape(1, 1), key_cache, value_cache, item_table, w_qkvu, w_out)


def solution(mesh):
    users = ("grp", "user")
    return jax.shard_map(
        functools.partial(body, mesh.shape["user"] // 2, mesh.shape["head"]),
        mesh=mesh,
        in_specs=(
            P(users, None),
            P(users),
            P(users, None, "head"),
            P(users, None, "head"),
            P("user", None),
            P(None, "head", None, None),
            P("head", None, None),
        ),
        out_specs=P(users, None),
        check_vma=False,
    )
```

```python
import functools

import jax
import jax.numpy as jnp
from jax import lax
from jax.experimental import pallas as pl
from jax.experimental.pallas import tpu as pltpu
from jax.sharding import PartitionSpec as P

MESH = pl.DeviceIdType.MESH
LAG = 2
NT = (((1,), (1,)), ((), ()))
TN = (((0,), (0,)), ((), ()))


def log2(n):
    assert n & (n - 1) == 0
    return n.bit_length() - 1


def silu(v):
    half = 0.5 * v
    return half + half * jnp.tanh(half)


def kernel(
    nz, nh, cap, ids_hbm, len_hbm, k_hbm, v_hbm, table_hbm, wq_hbm, wo_hbm, out_ref,
    ids_ref, len_ref, table, wq_in, wq, keys, values, wfull, req, req_in, rows, emb, gout, gat, slots, part,
    load_sem, req_send, req_recv, row_send, row_recv, fwd_send, fwd_recv, gat_send, gat_recv,
    w_send, w_recv, wp_send, wp_recv, s_send, s_recv,
):
    f32, bf16, i32 = jnp.float32, jnp.bfloat16, jnp.int32
    u, x = lax.axis_index("user"), lax.axis_index("head")
    z, c = u // 2, u % 2
    steps = nz // nh
    n = ids_hbm.shape[1]
    shard_rows, d_model = table.shape
    blocks = 2 * nh * steps
    own_class = (x + c * (nh // 2)) % nh

    def offset(quarter, j):
        half, odd = j // 2, j % 2
        return quarter + nh * (half + odd * (steps - 1 - 2 * half))

    def shard(j, core):
        quarter = (x + core * (nh // 2)) % nh
        return 2 * ((z + offset(quarter, j)) % nz) + core

    def requester(j, core):
        return 2 * ((z + nz - offset(own_class, j)) % nz) + core

    def head(d):
        return (x + d) % nh

    partner = u + 1 - 2 * c

    barrier = pltpu.get_barrier_semaphore()

    def greet(i, carry):
        j = steps - 1 - i
        for core in (0, 1):
            for user in (shard(j, core), requester(j, core)):

                @pl.when(user != u)
                def _():
                    pl.semaphore_signal(
                        barrier, inc=1, device_id={"user": user}, device_id_type=MESH
                    )

        return carry

    lax.fori_loop(0, steps, greet, 0)
    for d in range(1, nh):
        pl.semaphore_signal(barrier, inc=1, device_id={"head": head(d)}, device_id_type=MESH)
    pl.semaphore_signal(barrier, inc=1, device_id={"user": partner}, device_id_type=MESH)

    loads = [
        pltpu.make_async_copy(src, dst, load_sem.at[i])
        for i, (src, dst) in enumerate(
            (
                (table_hbm, table),
                (wq_hbm, wq_in),
                (k_hbm.at[0], keys),
                (v_hbm.at[0], values),
                (wo_hbm, wfull.at[x]),
                (ids_hbm, ids_ref),
                (len_hbm, len_ref),
            )
        )
    ]
    for load in loads[5:] + loads[:5]:
        load.start()
    loads[5].wait()

    ids = ids_ref[...]
    shard_of = ids >> log2(shard_rows)
    local = ids & (shard_rows - 1)
    core_of = shard_of & 1
    off = ((shard_of >> 1) - z) & (nz - 1)
    turn = off >> log2(nh)
    owner = (off - core_of * (nh // 2)) & (nh - 1)
    step_of = jnp.where(turn < steps // 2, 2 * turn, 2 * (steps - 1 - turn) + 1)
    block_of = (step_of * nh + owner) * 2 + core_of
    in_block = lax.broadcasted_iota(i32, (blocks, n), 0) == block_of
    one_hot = jnp.where(in_block, 1.0, 0.0).astype(bf16)
    before = lax.broadcasted_iota(i32, (n, n), 0) < lax.broadcasted_iota(i32, (n, n), 1)
    earlier = jnp.dot(
        one_hot, jnp.where(before, 1.0, 0.0).astype(bf16), preferred_element_type=f32
    )
    place = jnp.sum(jnp.where(in_block, earlier, 0.0), axis=0, keepdims=True).astype(i32)
    slots[...] = block_of * cap + place
    at_place = (lax.broadcasted_iota(i32, (128, n), 0) & (cap - 1)) == place
    high = jnp.where(at_place, (local >> 5).astype(f32), 0.0).astype(bf16)
    low = jnp.where(at_place, (local & 31).astype(f32), 0.0).astype(bf16)
    wanted = (
        lax.dot_general(one_hot, high, NT, preferred_element_type=f32) * 32.0
        + lax.dot_general(one_hot, low, NT, preferred_element_type=f32)
    ).astype(i32)
    for b in range(blocks):
        req[b] = wanted[b : b + 1]

    others = (own_class + nh - 1) // nh
    with jax.named_scope("barrier"):
        pl.semaphore_wait(barrier, 4 * steps + nh - 2 + 2 * others)

    def to_user(src, dst, send_sem, recv_sem, user):
        return pltpu.make_async_remote_copy(
            src_ref=src,
            dst_ref=dst,
            send_sem=send_sem,
            recv_sem=recv_sem,
            device_id={"user": user},
            device_id_type=MESH,
        )

    def to_head(src, dst, send_sem, recv_sem, d):
        return pltpu.make_async_remote_copy(
            src_ref=src,
            dst_ref=dst,
            send_sem=send_sem,
            recv_sem=recv_sem,
            device_id={"head": head(d)},
            device_id_type=MESH,
        )

    def start_unless_self(copy, src, dst, recv_sem, user):
        @pl.when(user != u)
        def _():
            copy.start()

        @pl.when(user == u)
        def _():
            pltpu.make_async_copy(src, dst, recv_sem).start()

    def request(j, core):
        user = shard(j, core)
        src, dst = req.at[(j * nh + x) * 2 + core], req_in.at[j, c]
        return to_user(src, dst, req_send.at[j, core], req_recv.at[j], user), src, dst, user

    def ask(i, carry):
        j = steps - 1 - i
        for core in (0, 1):
            copy, src, dst, user = request(j, core)
            start_unless_self(copy, src, dst, req_recv.at[j], user)
        return carry

    with jax.named_scope("ask"):
        lax.fori_loop(0, steps, ask, 0)

    def half_out(d):
        return to_head(wo_hbm.at[c], wfull.at[x, c], w_send.at[d - 1], w_recv.at[d - 1], d)

    for d in range(1, nh):
        half_out(d).start()

    loads[0].wait()

    def answer(j, core):
        user = requester(j, core)
        src, dst = rows.at[j, core], emb.at[j, x, c]
        return to_user(src, dst, row_send.at[j, core], row_recv.at[j], user), src, dst, user

    def serve(j, carry):
        with jax.named_scope("req_wait"):
            pltpu.make_async_copy(req_in.at[j], req_in.at[j], req_recv.at[j]).wait()
        lane = lax.broadcasted_iota(i32, (1, 2 * cap), 1)
        both = jnp.where(lane < cap, req_in[j, 0][:, : 2 * cap], req_in[j, 1][:, : 2 * cap])
        pick = lax.broadcasted_iota(i32, (shard_rows, 2 * cap), 0) == both
        found = lax.dot_general(
            jnp.where(pick, 1.0, 0.0).astype(bf16), table[...], TN, preferred_element_type=f32
        )
        rows[j] = found.astype(bf16).reshape(2, cap, d_model)
        for core in (0, 1):
            copy, src, dst, user = answer(j, core)
            start_unless_self(copy, src, dst, row_recv.at[j], user)
        return carry

    lax.fori_loop(0, steps, serve, 0)

    def half_on(d):
        piece = wfull.at[(x + nh - d) % nh, c]
        return to_user(piece, piece, wp_send.at[d - 1], wp_recv.at[d - 1], partner)

    for d in range(1, nh):
        piece = wfull.at[(x + nh - d) % nh, c]
        with jax.named_scope("w_wait"):
            pltpu.make_async_copy(piece, piece, w_recv.at[d - 1]).wait()
        half_on(d).start()

    for load in loads[1:5] + loads[6:]:
        load.wait()
    span = 128

    def relay_weights(i, carry):
        at = pl.ds(pl.multiple_of(i * span, span), span)
        wq[at, :] = wq_in[at].reshape(span, wq.shape[1])
        return carry

    with jax.named_scope("relay"):
        lax.fori_loop(0, d_model // span, relay_weights, 0)

    length = len_ref[0, 0]
    head_size = 128
    heads_here = keys.shape[1] // head_size
    prefix = keys.shape[0]
    scale = head_size ** (-0.5)
    per_token = 1.0 / (jnp.zeros((1, 1), f32) + (length + 1).astype(f32))
    inside = lax.broadcasted_iota(i32, (1, prefix), 1) < length
    factor = jnp.where(inside, (0.5 * scale) * per_token, 0.0)

    def forward(j, d):
        mine = emb.at[j, x]
        return to_head(mine, mine, fwd_send.at[j, d - 1], fwd_recv.at[j, d - 1], d)

    def give(j, d):
        return to_head(
            gout.at[j, head(d)], gat.at[j, x], gat_send.at[j, d - 1], gat_recv.at[j, d - 1], d
        )

    def compute(j):
        for d in range(1, nh):
            theirs = emb.at[j, (x + nh - d) % nh]
            with jax.named_scope("fwd_wait"):
                pltpu.make_async_copy(theirs, theirs, fwd_recv.at[j, d - 1]).wait()
        embedded = emb[j].reshape(nh * 2 * cap, d_model)
        projected = jnp.dot(embedded, wq[...], preferred_element_type=f32)
        activated = silu(projected).astype(bf16)
        for h in range(heads_here):
            columns = slice(h * head_size, (h + 1) * head_size)
            queries, own_keys, own_values, gates = (
                activated[:, (4 * h + i) * head_size : (4 * h + i + 1) * head_size]
                for i in range(4)
            )
            raw = lax.dot_general(queries, keys[:, columns], NT, preferred_element_type=f32)
            weights = (raw * factor) * (1.0 + jnp.tanh(raw * (0.5 * scale)))
            attended = jnp.dot(
                weights.astype(bf16), values[:, columns], preferred_element_type=f32
            )
            own_dot = jnp.sum(
                queries.astype(f32) * own_keys.astype(f32), axis=1, keepdims=True
            )
            own_weight = silu(own_dot * scale) * per_token
            attended = attended + own_weight * own_values.astype(f32)
            mean_square = jnp.mean(attended * attended, axis=1, keepdims=True)
            gated = attended * lax.rsqrt(mean_square + 1e-06) * gates.astype(f32)
            gout[j, :, :, columns] = gated.astype(bf16).reshape(nh, 2 * cap, head_size)
        for d in range(1, nh):
            give(j, d).start()

    def stage(j, carry):
        @pl.when(j < steps)
        def _():
            mine = emb.at[j, x]
            with jax.named_scope("row_wait"):
                pltpu.make_async_copy(mine, mine, row_recv.at[j]).wait()
            for d in range(1, nh):
                forward(j, d).start()

        @pl.when(j >= LAG)
        def _():
            compute(j - LAG)

        return carry

    lax.fori_loop(0, steps + LAG, stage, 0)

    for d in range(1, nh):
        piece = wfull.at[(x + nh - d) % nh, 1 - c]
        with jax.named_scope("wp_wait"):
            pltpu.make_async_copy(piece, piece, wp_recv.at[d - 1]).wait()

    def collect(j, carry):
        for d in range(1, nh):
            theirs = gat.at[j, (x + nh - d) % nh]
            with jax.named_scope("gat_wait"):
                pltpu.make_async_copy(theirs, theirs, gat_recv.at[j, d - 1]).wait()
        gat[j, x] = gout[j, x]
        return carry

    lax.fori_loop(0, steps, collect, 0)
    own = steps * 2 * cap
    width = gat.shape[-1]
    summed = jnp.zeros((own, d_model), f32)
    for y in range(nh):
        summed = summed + jnp.dot(
            gat[:, y].reshape(own, width),
            wfull[y].reshape(width, d_model),
            preferred_element_type=f32,
        )
    mine = emb[:, pl.ds(x, 1)].reshape(own, d_model).astype(f32)
    inner = jnp.sum(summed * mine, axis=1, keepdims=True)
    square = jnp.sum(summed * summed, axis=1, keepdims=True)
    score = inner * d_model ** (-0.5) * lax.rsqrt(square / d_model + 1e-06)
    row = lax.broadcasted_iota(i32, (own, n), 0)
    slot = ((row >> log2(2 * cap)) * nh + x) * (2 * cap) + (row & (2 * cap - 1))
    part[...] = jnp.sum(jnp.where(slot == slots[...], score, 0.0), axis=0, keepdims=True)

    def share(d):
        return to_head(part, out_ref.at[x], s_send.at[d - 1], s_recv.at[d - 1], d)

    for d in range(1, nh):
        share(d).start()
    keep = pltpu.make_async_copy(part, out_ref.at[x], load_sem.at[0])
    keep.start()

    def drain(j, carry):
        for core in (0, 1):
            for make in (request, answer):
                copy, _, _, user = make(j, core)

                @pl.when(user != u)
                def _():
                    copy.wait_send()

        for d in range(1, nh):
            forward(j, d).wait_send()
            give(j, d).wait_send()
        return carry

    with jax.named_scope("drain"):
        lax.fori_loop(0, steps, drain, 0)
    for d in range(1, nh):
        half_out(d).wait_send()
        half_on(d).wait_send()
    keep.wait()
    for d in range(1, nh):
        share(d).wait_send()
        theirs = out_ref.at[(x + nh - d) % nh]
        with jax.named_scope("s_wait"):
            pltpu.make_async_copy(theirs, theirs, s_recv.at[d - 1]).wait()


def body(nz, nh, cand_ids, prefix_len, key_cache, value_cache, item_table, w_qkvu, w_out):
    n = cand_ids.shape[1]
    prefix, width = key_cache.shape[1:]
    shard_rows, d_model = item_table.shape
    steps = nz // nh
    blocks = 2 * nz
    cap = 2 * n // blocks
    bf16, dma = jnp.bfloat16, pltpu.SemaphoreType.DMA
    hbm = pl.BlockSpec(memory_space=pl.ANY)
    wq_width = w_qkvu.size // d_model
    parts = pl.pallas_call(
        functools.partial(kernel, nz, nh, cap),
        out_shape=jax.ShapeDtypeStruct((nh, 1, n), jnp.float32),
        in_specs=[hbm] * 7,
        out_specs=hbm,
        scratch_shapes=[
            pltpu.VMEM((1, n), jnp.int32),
            pltpu.SMEM((1, 1), jnp.int32),
            pltpu.VMEM((shard_rows, d_model), bf16),
            pltpu.VMEM(w_qkvu.shape, bf16),
            pltpu.VMEM((d_model, wq_width), bf16),
            pltpu.VMEM((prefix, width), bf16),
            pltpu.VMEM((prefix, width), bf16),
            pltpu.VMEM((nh, *w_out.shape), bf16),
            pltpu.VMEM((blocks, 1, 128), jnp.int32),
            pltpu.VMEM((steps, 2, 1, 128), jnp.int32),
            pltpu.VMEM((steps, 2, cap, d_model), bf16),
            pltpu.VMEM((steps, nh, 2, cap, d_model), bf16),
            pltpu.VMEM((steps, nh, 2 * cap, width), bf16),
            pltpu.VMEM((steps, nh, 2 * cap, width), bf16),
            pltpu.VMEM((1, n), jnp.int32),
            pltpu.VMEM((1, n), jnp.float32),
            dma((7,)),
            dma((steps, 2)),
            dma((steps,)),
            dma((steps, 2)),
            dma((steps,)),
            dma((steps, nh - 1)),
            dma((steps, nh - 1)),
            dma((steps, nh - 1)),
            dma((steps, nh - 1)),
            dma((nh - 1,)),
            dma((nh - 1,)),
            dma((nh - 1,)),
            dma((nh - 1,)),
            dma((nh - 1,)),
            dma((nh - 1,)),
        ],
        compiler_params=pltpu.CompilerParams(
            collective_id=0, has_side_effects=True, vmem_limit_bytes=67_043_328
        ),
    )(cand_ids, prefix_len.reshape(1, 1), key_cache, value_cache, item_table, w_qkvu, w_out)
    return jnp.sum(parts, axis=0)


def solution(mesh):
    users = ("grp", "user")
    return jax.shard_map(
        functools.partial(body, mesh.shape["user"] // 2, mesh.shape["head"]),
        mesh=mesh,
        in_specs=(
            P(users, None),
            P(users),
            P(users, None, "head"),
            P(users, None, "head"),
            P("user", None),
            P(None, "head", None, None),
            P("head", None, None),
        ),
        out_specs=P(users, None),
        check_vma=False,
    )
```

```python
import functools

import jax
import jax.numpy as jnp
from jax import lax
from jax.experimental import pallas as pl
from jax.experimental.pallas import tpu as pltpu
from jax.sharding import PartitionSpec as P

MESH = pl.DeviceIdType.MESH
LAG = 2
NT = (((1,), (1,)), ((), ()))
TN = (((0,), (0,)), ((), ()))


def log2(n):
    assert n & (n - 1) == 0
    return n.bit_length() - 1


def silu(v):
    half = 0.5 * v
    return half + half * jnp.tanh(half)


def kernel(
    nz, nh, cap, ids_hbm, len_hbm, k_hbm, v_hbm, table_hbm, wq_hbm, wo_hbm, out_ref,
    ids_ref, len_ref, table, wq_in, wq, keys, values, wfull, req, req_in, rows, emb, gout, gat, slots, part,
    load_sem, req_send, req_recv, row_send, row_recv, fwd_send, fwd_recv, gat_send, gat_recv,
    w_send, w_recv, wp_send, wp_recv, s_send, s_recv,
):
    f32, bf16, i32 = jnp.float32, jnp.bfloat16, jnp.int32
    u, x = lax.axis_index("user"), lax.axis_index("head")
    z, c = u // 2, u % 2
    steps = nz // nh
    n = ids_hbm.shape[1]
    shard_rows, d_model = table.shape
    blocks = 2 * nh * steps
    own_class = (x + c * (nh // 2)) % nh

    def offset(quarter, j):
        flip = quarter // (nh // 2 + 1)
        half, back = j // 2, (j + flip) % 2
        return quarter + nh * (half + back * (steps - 1 - 2 * half))

    def shard(j, core):
        quarter = (x + core * (nh // 2)) % nh
        return 2 * ((z + offset(quarter, j)) % nz) + core

    def requester(j, core):
        return 2 * ((z + nz - offset(own_class, j)) % nz) + core

    def head(d):
        return (x + d) % nh

    partner = u + 1 - 2 * c

    barrier = pltpu.get_barrier_semaphore()

    def greet(j, carry):
        for core in (0, 1):
            for user in (shard(j, core), requester(j, core)):

                @pl.when(user != u)
                def _():
                    pl.semaphore_signal(
                        barrier, inc=1, device_id={"user": user}, device_id_type=MESH
                    )

        return carry

    lax.fori_loop(0, steps, greet, 0)
    for d in range(1, nh):
        pl.semaphore_signal(barrier, inc=1, device_id={"head": head(d)}, device_id_type=MESH)
    pl.semaphore_signal(barrier, inc=1, device_id={"user": partner}, device_id_type=MESH)

    loads = [
        pltpu.make_async_copy(src, dst, load_sem.at[i])
        for i, (src, dst) in enumerate(
            (
                (table_hbm, table),
                (wq_hbm, wq_in),
                (k_hbm.at[0], keys),
                (v_hbm.at[0], values),
                (wo_hbm, wfull.at[x]),
                (ids_hbm, ids_ref),
                (len_hbm, len_ref),
            )
        )
    ]
    for load in loads[5:] + loads[:5]:
        load.start()
    loads[5].wait()

    ids = ids_ref[...]
    shard_of = ids >> log2(shard_rows)
    local = ids & (shard_rows - 1)
    core_of = shard_of & 1
    off = ((shard_of >> 1) - z) & (nz - 1)
    turn = off >> log2(nh)
    quarter_of = off & (nh - 1)
    owner = (quarter_of - core_of * (nh // 2)) & (nh - 1)
    flip_of = jnp.where(quarter_of > nh // 2, 1, 0)
    step_of = jnp.where(
        turn < steps // 2, 2 * turn + flip_of, 2 * (steps - 1 - turn) + 1 - flip_of
    )
    block_of = (step_of * nh + owner) * 2 + core_of
    in_block = lax.broadcasted_iota(i32, (blocks, n), 0) == block_of
    one_hot = jnp.where(in_block, 1.0, 0.0).astype(bf16)
    before = lax.broadcasted_iota(i32, (n, n), 0) < lax.broadcasted_iota(i32, (n, n), 1)
    earlier = jnp.dot(
        one_hot, jnp.where(before, 1.0, 0.0).astype(bf16), preferred_element_type=f32
    )
    place = jnp.sum(jnp.where(in_block, earlier, 0.0), axis=0, keepdims=True).astype(i32)
    slots[...] = block_of * cap + place
    at_place = (lax.broadcasted_iota(i32, (128, n), 0) & (cap - 1)) == place
    high = jnp.where(at_place, (local >> 5).astype(f32), 0.0).astype(bf16)
    low = jnp.where(at_place, (local & 31).astype(f32), 0.0).astype(bf16)
    wanted = (
        lax.dot_general(one_hot, high, NT, preferred_element_type=f32) * 32.0
        + lax.dot_general(one_hot, low, NT, preferred_element_type=f32)
    ).astype(i32)
    for b in range(blocks):
        req[b] = wanted[b : b + 1]

    others = (own_class + nh - 1) // nh
    with jax.named_scope("barrier"):
        pl.semaphore_wait(barrier, 4 * steps + nh - 2 + 2 * others)

    def to_user(src, dst, send_sem, recv_sem, user):
        return pltpu.make_async_remote_copy(
            src_ref=src,
            dst_ref=dst,
            send_sem=send_sem,
            recv_sem=recv_sem,
            device_id={"user": user},
            device_id_type=MESH,
        )

    def to_head(src, dst, send_sem, recv_sem, d):
        return pltpu.make_async_remote_copy(
            src_ref=src,
            dst_ref=dst,
            send_sem=send_sem,
            recv_sem=recv_sem,
            device_id={"head": head(d)},
            device_id_type=MESH,
        )

    def start_unless_self(copy, src, dst, recv_sem, user):
        @pl.when(user != u)
        def _():
            copy.start()

        @pl.when(user == u)
        def _():
            pltpu.make_async_copy(src, dst, recv_sem).start()

    def request(j, core):
        user = shard(j, core)
        src, dst = req.at[(j * nh + x) * 2 + core], req_in.at[j, c]
        return to_user(src, dst, req_send.at[j, core], req_recv.at[j], user), src, dst, user

    def ask(j, carry):
        for core in (0, 1):
            copy, src, dst, user = request(j, core)
            start_unless_self(copy, src, dst, req_recv.at[j], user)
        return carry

    with jax.named_scope("ask"):
        lax.fori_loop(0, steps, ask, 0)

    def half_out(d):
        return to_head(wo_hbm.at[c], wfull.at[x, c], w_send.at[d - 1], w_recv.at[d - 1], d)

    for d in range(1, nh):
        half_out(d).start()

    loads[0].wait()

    def answer(j, core):
        user = requester(j, core)
        src, dst = rows.at[j, core], emb.at[j, x, c]
        return to_user(src, dst, row_send.at[j, core], row_recv.at[j], user), src, dst, user

    def serve(j, carry):
        with jax.named_scope("req_wait"):
            pltpu.make_async_copy(req_in.at[j], req_in.at[j], req_recv.at[j]).wait()
        lane = lax.broadcasted_iota(i32, (1, 2 * cap), 1)
        both = jnp.where(lane < cap, req_in[j, 0][:, : 2 * cap], req_in[j, 1][:, : 2 * cap])
        pick = lax.broadcasted_iota(i32, (shard_rows, 2 * cap), 0) == both
        found = lax.dot_general(
            jnp.where(pick, 1.0, 0.0).astype(bf16), table[...], TN, preferred_element_type=f32
        )
        rows[j] = found.astype(bf16).reshape(2, cap, d_model)
        for core in (0, 1):
            copy, src, dst, user = answer(j, core)
            start_unless_self(copy, src, dst, row_recv.at[j], user)
        return carry

    lax.fori_loop(0, steps, serve, 0)

    def half_on(d):
        piece = wfull.at[(x + nh - d) % nh, c]
        return to_user(piece, piece, wp_send.at[d - 1], wp_recv.at[d - 1], partner)

    for d in range(1, nh):
        piece = wfull.at[(x + nh - d) % nh, c]
        with jax.named_scope("w_wait"):
            pltpu.make_async_copy(piece, piece, w_recv.at[d - 1]).wait()
        half_on(d).start()

    for load in loads[1:5] + loads[6:]:
        load.wait()
    span = 128

    def relay_weights(i, carry):
        at = pl.ds(pl.multiple_of(i * span, span), span)
        wq[at, :] = wq_in[at].reshape(span, wq.shape[1])
        return carry

    with jax.named_scope("relay"):
        lax.fori_loop(0, d_model // span, relay_weights, 0)

    length = len_ref[0, 0]
    head_size = 128
    heads_here = keys.shape[1] // head_size
    prefix = keys.shape[0]
    scale = head_size ** (-0.5)
    per_token = 1.0 / (jnp.zeros((1, 1), f32) + (length + 1).astype(f32))
    inside = lax.broadcasted_iota(i32, (1, prefix), 1) < length
    factor = jnp.where(inside, (0.5 * scale) * per_token, 0.0)

    def forward(j, d):
        mine = emb.at[j, x]
        return to_head(mine, mine, fwd_send.at[j, d - 1], fwd_recv.at[j, d - 1], d)

    def give(j, d):
        return to_head(
            gout.at[j, head(d)], gat.at[j, x], gat_send.at[j, d - 1], gat_recv.at[j, d - 1], d
        )

    def compute(j):
        for d in range(1, nh):
            theirs = emb.at[j, (x + nh - d) % nh]
            with jax.named_scope("fwd_wait"):
                pltpu.make_async_copy(theirs, theirs, fwd_recv.at[j, d - 1]).wait()
        embedded = emb[j].reshape(nh * 2 * cap, d_model)
        projected = jnp.dot(embedded, wq[...], preferred_element_type=f32)
        activated = silu(projected).astype(bf16)
        for h in range(heads_here):
            columns = slice(h * head_size, (h + 1) * head_size)
            queries, own_keys, own_values, gates = (
                activated[:, (4 * h + i) * head_size : (4 * h + i + 1) * head_size]
                for i in range(4)
            )
            raw = lax.dot_general(queries, keys[:, columns], NT, preferred_element_type=f32)
            weights = (raw * factor) * (1.0 + jnp.tanh(raw * (0.5 * scale)))
            attended = jnp.dot(
                weights.astype(bf16), values[:, columns], preferred_element_type=f32
            )
            own_dot = jnp.sum(
                queries.astype(f32) * own_keys.astype(f32), axis=1, keepdims=True
            )
            own_weight = silu(own_dot * scale) * per_token
            attended = attended + own_weight * own_values.astype(f32)
            mean_square = jnp.mean(attended * attended, axis=1, keepdims=True)
            gated = attended * lax.rsqrt(mean_square + 1e-06) * gates.astype(f32)
            gout[j, :, :, columns] = gated.astype(bf16).reshape(nh, 2 * cap, head_size)
        for d in range(1, nh):
            give(j, d).start()

    def stage(j, carry):
        @pl.when(j < steps)
        def _():
            mine = emb.at[j, x]
            with jax.named_scope("row_wait"):
                pltpu.make_async_copy(mine, mine, row_recv.at[j]).wait()
            for d in range(1, nh):
                forward(j, d).start()

        @pl.when(j >= LAG)
        def _():
            compute(j - LAG)

        return carry

    lax.fori_loop(0, steps + LAG, stage, 0)

    for d in range(1, nh):
        piece = wfull.at[(x + nh - d) % nh, 1 - c]
        with jax.named_scope("wp_wait"):
            pltpu.make_async_copy(piece, piece, wp_recv.at[d - 1]).wait()

    def collect(j, carry):
        for d in range(1, nh):
            theirs = gat.at[j, (x + nh - d) % nh]
            with jax.named_scope("gat_wait"):
                pltpu.make_async_copy(theirs, theirs, gat_recv.at[j, d - 1]).wait()
        gat[j, x] = gout[j, x]
        return carry

    lax.fori_loop(0, steps, collect, 0)
    own = steps * 2 * cap
    width = gat.shape[-1]
    summed = jnp.zeros((own, d_model), f32)
    for y in range(nh):
        summed = summed + jnp.dot(
            gat[:, y].reshape(own, width),
            wfull[y].reshape(width, d_model),
            preferred_element_type=f32,
        )
    mine = emb[:, pl.ds(x, 1)].reshape(own, d_model).astype(f32)
    inner = jnp.sum(summed * mine, axis=1, keepdims=True)
    square = jnp.sum(summed * summed, axis=1, keepdims=True)
    score = inner * d_model ** (-0.5) * lax.rsqrt(square / d_model + 1e-06)
    row = lax.broadcasted_iota(i32, (own, n), 0)
    slot = ((row >> log2(2 * cap)) * nh + x) * (2 * cap) + (row & (2 * cap - 1))
    part[...] = jnp.sum(jnp.where(slot == slots[...], score, 0.0), axis=0, keepdims=True)

    def share(d):
        return to_head(part, out_ref.at[x], s_send.at[d - 1], s_recv.at[d - 1], d)

    for d in range(1, nh):
        share(d).start()
    keep = pltpu.make_async_copy(part, out_ref.at[x], load_sem.at[0])
    keep.start()

    def drain(j, carry):
        for core in (0, 1):
            for make in (request, answer):
                copy, _, _, user = make(j, core)

                @pl.when(user != u)
                def _():
                    copy.wait_send()

        for d in range(1, nh):
            forward(j, d).wait_send()
            give(j, d).wait_send()
        return carry

    with jax.named_scope("drain"):
        lax.fori_loop(0, steps, drain, 0)
    for d in range(1, nh):
        half_out(d).wait_send()
        half_on(d).wait_send()
    keep.wait()
    for d in range(1, nh):
        share(d).wait_send()
        theirs = out_ref.at[(x + nh - d) % nh]
        with jax.named_scope("s_wait"):
            pltpu.make_async_copy(theirs, theirs, s_recv.at[d - 1]).wait()


def body(nz, nh, cand_ids, prefix_len, key_cache, value_cache, item_table, w_qkvu, w_out):
    n = cand_ids.shape[1]
    prefix, width = key_cache.shape[1:]
    shard_rows, d_model = item_table.shape
    steps = nz // nh
    blocks = 2 * nz
    cap = 2 * n // blocks
    bf16, dma = jnp.bfloat16, pltpu.SemaphoreType.DMA
    hbm = pl.BlockSpec(memory_space=pl.ANY)
    wq_width = w_qkvu.size // d_model
    parts = pl.pallas_call(
        functools.partial(kernel, nz, nh, cap),
        out_shape=jax.ShapeDtypeStruct((nh, 1, n), jnp.float32),
        in_specs=[hbm] * 7,
        out_specs=hbm,
        scratch_shapes=[
            pltpu.VMEM((1, n), jnp.int32),
            pltpu.SMEM((1, 1), jnp.int32),
            pltpu.VMEM((shard_rows, d_model), bf16),
            pltpu.VMEM(w_qkvu.shape, bf16),
            pltpu.VMEM((d_model, wq_width), bf16),
            pltpu.VMEM((prefix, width), bf16),
            pltpu.VMEM((prefix, width), bf16),
            pltpu.VMEM((nh, *w_out.shape), bf16),
            pltpu.VMEM((blocks, 1, 128), jnp.int32),
            pltpu.VMEM((steps, 2, 1, 128), jnp.int32),
            pltpu.VMEM((steps, 2, cap, d_model), bf16),
            pltpu.VMEM((steps, nh, 2, cap, d_model), bf16),
            pltpu.VMEM((steps, nh, 2 * cap, width), bf16),
            pltpu.VMEM((steps, nh, 2 * cap, width), bf16),
            pltpu.VMEM((1, n), jnp.int32),
            pltpu.VMEM((1, n), jnp.float32),
            dma((7,)),
            dma((steps, 2)),
            dma((steps,)),
            dma((steps, 2)),
            dma((steps,)),
            dma((steps, nh - 1)),
            dma((steps, nh - 1)),
            dma((steps, nh - 1)),
            dma((steps, nh - 1)),
            dma((nh - 1,)),
            dma((nh - 1,)),
            dma((nh - 1,)),
            dma((nh - 1,)),
            dma((nh - 1,)),
            dma((nh - 1,)),
        ],
        compiler_params=pltpu.CompilerParams(
            collective_id=0, has_side_effects=True, vmem_limit_bytes=67_043_328
        ),
    )(cand_ids, prefix_len.reshape(1, 1), key_cache, value_cache, item_table, w_qkvu, w_out)
    return jnp.sum(parts, axis=0)


def solution(mesh):
    users = ("grp", "user")
    return jax.shard_map(
        functools.partial(body, mesh.shape["user"] // 2, mesh.shape["head"]),
        mesh=mesh,
        in_specs=(
            P(users, None),
            P(users),
            P(users, None, "head"),
            P(users, None, "head"),
            P("user", None),
            P(None, "head", None, None),
            P("head", None, None),
        ),
        out_specs=P(users, None),
        check_vma=False,
    )
```

```python
import functools

import jax
import jax.numpy as jnp
from jax import lax
from jax.experimental import pallas as pl
from jax.experimental.pallas import tpu as pltpu
from jax.sharding import PartitionSpec as P

MESH = pl.DeviceIdType.MESH
LAG = 2
NT = (((1,), (1,)), ((), ()))
TN = (((0,), (0,)), ((), ()))


def log2(n):
    assert n & (n - 1) == 0
    return n.bit_length() - 1


def silu(v):
    half = 0.5 * v
    return half + half * jnp.tanh(half)


def kernel(
    nz, nh, cap, ids_hbm, len_hbm, k_hbm, v_hbm, table_hbm, wq_hbm, wo_hbm, out_ref,
    ids_ref, len_ref, table, wq_in, wq, keys, values, wfull, req, req_in, rows, emb, gout, gat, slots, part,
    load_sem, req_send, req_recv, row_send, row_recv, fwd_send, fwd_recv, gat_send, gat_recv,
    w_send, w_recv, wp_send, wp_recv, s_send, s_recv,
):
    f32, bf16, i32 = jnp.float32, jnp.bfloat16, jnp.int32
    u, x = lax.axis_index("user"), lax.axis_index("head")
    z, c = u // 2, u % 2
    steps = nz // nh
    n = ids_hbm.shape[1]
    shard_rows, d_model = table.shape
    blocks = 2 * nh * steps
    own_class = (x + c * (nh // 2)) % nh

    def offset(quarter, j):
        flip = quarter // (nh // 2 + 1)
        half, back = j // 2, (j + flip) % 2
        return quarter + nh * (half + back * (steps - 1 - 2 * half))

    def shard(j, core):
        quarter = (x + core * (nh // 2)) % nh
        return 2 * ((z + offset(quarter, j)) % nz) + core

    def requester(j, core):
        return 2 * ((z + nz - offset(own_class, j)) % nz) + core

    def head(d):
        return (x + d) % nh

    partner = u + 1 - 2 * c
    farthest_first = sorted(range(1, nh), key=lambda d: -min(d, nh - d))

    barrier = pltpu.get_barrier_semaphore()

    def greet(j, carry):
        for core in (0, 1):
            for user in (shard(j, core), requester(j, core)):

                @pl.when(user != u)
                def _():
                    pl.semaphore_signal(
                        barrier, inc=1, device_id={"user": user}, device_id_type=MESH
                    )

        return carry

    lax.fori_loop(0, steps, greet, 0)
    for d in range(1, nh):
        pl.semaphore_signal(barrier, inc=1, device_id={"head": head(d)}, device_id_type=MESH)
    pl.semaphore_signal(barrier, inc=1, device_id={"user": partner}, device_id_type=MESH)

    loads = [
        pltpu.make_async_copy(src, dst, load_sem.at[i])
        for i, (src, dst) in enumerate(
            (
                (table_hbm, table),
                (wq_hbm, wq_in),
                (k_hbm.at[0], keys),
                (v_hbm.at[0], values),
                (wo_hbm, wfull.at[x]),
                (ids_hbm, ids_ref),
                (len_hbm, len_ref),
            )
        )
    ]
    for load in loads[5:] + loads[:5]:
        load.start()
    loads[5].wait()

    ids = ids_ref[...]
    shard_of = ids >> log2(shard_rows)
    local = ids & (shard_rows - 1)
    core_of = shard_of & 1
    off = ((shard_of >> 1) - z) & (nz - 1)
    turn = off >> log2(nh)
    quarter_of = off & (nh - 1)
    owner = (quarter_of - core_of * (nh // 2)) & (nh - 1)
    flip_of = jnp.where(quarter_of > nh // 2, 1, 0)
    step_of = jnp.where(
        turn < steps // 2, 2 * turn + flip_of, 2 * (steps - 1 - turn) + 1 - flip_of
    )
    block_of = (step_of * nh + owner) * 2 + core_of
    in_block = lax.broadcasted_iota(i32, (blocks, n), 0) == block_of
    one_hot = jnp.where(in_block, 1.0, 0.0).astype(bf16)
    before = lax.broadcasted_iota(i32, (n, n), 0) < lax.broadcasted_iota(i32, (n, n), 1)
    earlier = jnp.dot(
        one_hot, jnp.where(before, 1.0, 0.0).astype(bf16), preferred_element_type=f32
    )
    place = jnp.sum(jnp.where(in_block, earlier, 0.0), axis=0, keepdims=True).astype(i32)
    slots[...] = block_of * cap + place
    at_place = (lax.broadcasted_iota(i32, (128, n), 0) & (cap - 1)) == place
    high = jnp.where(at_place, (local >> 5).astype(f32), 0.0).astype(bf16)
    low = jnp.where(at_place, (local & 31).astype(f32), 0.0).astype(bf16)
    wanted = (
        lax.dot_general(one_hot, high, NT, preferred_element_type=f32) * 32.0
        + lax.dot_general(one_hot, low, NT, preferred_element_type=f32)
    ).astype(i32)
    for b in range(blocks):
        req[b] = wanted[b : b + 1]

    others = (own_class + nh - 1) // nh
    with jax.named_scope("barrier"):
        pl.semaphore_wait(barrier, 4 * steps + nh - 2 + 2 * others)

    def to_user(src, dst, send_sem, recv_sem, user):
        return pltpu.make_async_remote_copy(
            src_ref=src,
            dst_ref=dst,
            send_sem=send_sem,
            recv_sem=recv_sem,
            device_id={"user": user},
            device_id_type=MESH,
        )

    def to_head(src, dst, send_sem, recv_sem, d):
        return pltpu.make_async_remote_copy(
            src_ref=src,
            dst_ref=dst,
            send_sem=send_sem,
            recv_sem=recv_sem,
            device_id={"head": head(d)},
            device_id_type=MESH,
        )

    def start_unless_self(copy, src, dst, recv_sem, user):
        @pl.when(user != u)
        def _():
            copy.start()

        @pl.when(user == u)
        def _():
            pltpu.make_async_copy(src, dst, recv_sem).start()

    def request(j, core):
        user = shard(j, core)
        src, dst = req.at[(j * nh + x) * 2 + core], req_in.at[j, c]
        return to_user(src, dst, req_send.at[j, core], req_recv.at[j], user), src, dst, user

    def ask(j, carry):
        for core in (0, 1):
            copy, src, dst, user = request(j, core)
            start_unless_self(copy, src, dst, req_recv.at[j], user)
        return carry

    with jax.named_scope("ask"):
        lax.fori_loop(0, steps, ask, 0)

    def half_out(d):
        return to_head(wo_hbm.at[c], wfull.at[x, c], w_send.at[d - 1], w_recv.at[d - 1], d)

    for d in range(1, nh):
        half_out(d).start()

    loads[0].wait()

    def answer(j, core):
        user = requester(j, core)
        src, dst = rows.at[j, core], emb.at[j, x, c]
        return to_user(src, dst, row_send.at[j, core], row_recv.at[j], user), src, dst, user

    def serve(j, carry):
        with jax.named_scope("req_wait"):
            pltpu.make_async_copy(req_in.at[j], req_in.at[j], req_recv.at[j]).wait()
        lane = lax.broadcasted_iota(i32, (1, 2 * cap), 1)
        both = jnp.where(lane < cap, req_in[j, 0][:, : 2 * cap], req_in[j, 1][:, : 2 * cap])
        pick = lax.broadcasted_iota(i32, (shard_rows, 2 * cap), 0) == both
        found = lax.dot_general(
            jnp.where(pick, 1.0, 0.0).astype(bf16), table[...], TN, preferred_element_type=f32
        )
        rows[j] = found.astype(bf16).reshape(2, cap, d_model)
        for core in (0, 1):
            copy, src, dst, user = answer(j, core)
            start_unless_self(copy, src, dst, row_recv.at[j], user)
        return carry

    lax.fori_loop(0, steps, serve, 0)

    def half_on(d):
        piece = wfull.at[(x + nh - d) % nh, c]
        return to_user(piece, piece, wp_send.at[d - 1], wp_recv.at[d - 1], partner)

    for d in range(1, nh):
        piece = wfull.at[(x + nh - d) % nh, c]
        with jax.named_scope("w_wait"):
            pltpu.make_async_copy(piece, piece, w_recv.at[d - 1]).wait()
        half_on(d).start()

    for load in loads[1:5] + loads[6:]:
        load.wait()
    span = 128

    def relay_weights(i, carry):
        at = pl.ds(pl.multiple_of(i * span, span), span)
        wq[at, :] = wq_in[at].reshape(span, wq.shape[1])
        return carry

    with jax.named_scope("relay"):
        lax.fori_loop(0, d_model // span, relay_weights, 0)

    length = len_ref[0]
    head_size = 128
    heads_here = keys.shape[1] // head_size
    prefix = keys.shape[0]
    scale = head_size ** (-0.5)
    per_token = 1.0 / (jnp.zeros((1, 1), f32) + (length + 1).astype(f32))
    inside = lax.broadcasted_iota(i32, (1, prefix), 1) < length
    factor = jnp.where(inside, (0.5 * scale) * per_token, 0.0)

    def forward(j, d):
        mine = emb.at[j, x]
        return to_head(mine, mine, fwd_send.at[j, d - 1], fwd_recv.at[j, d - 1], d)

    def give(j, d):
        return to_head(
            gout.at[j, head(d)], gat.at[j, x], gat_send.at[j, d - 1], gat_recv.at[j, d - 1], d
        )

    def compute(j):
        for d in range(1, nh):
            theirs = emb.at[j, (x + nh - d) % nh]
            with jax.named_scope("fwd_wait"):
                pltpu.make_async_copy(theirs, theirs, fwd_recv.at[j, d - 1]).wait()
        embedded = emb[j].reshape(nh * 2 * cap, d_model)
        projected = jnp.dot(embedded, wq[...], preferred_element_type=f32)
        activated = silu(projected).astype(bf16)
        for h in range(heads_here):
            columns = slice(h * head_size, (h + 1) * head_size)
            queries, own_keys, own_values, gates = (
                activated[:, (4 * h + i) * head_size : (4 * h + i + 1) * head_size]
                for i in range(4)
            )
            raw = lax.dot_general(queries, keys[:, columns], NT, preferred_element_type=f32)
            weights = (raw * factor) * (1.0 + jnp.tanh(raw * (0.5 * scale)))
            attended = jnp.dot(
                weights.astype(bf16), values[:, columns], preferred_element_type=f32
            )
            own_dot = jnp.sum(
                queries.astype(f32) * own_keys.astype(f32), axis=1, keepdims=True
            )
            own_weight = silu(own_dot * scale) * per_token
            attended = attended + own_weight * own_values.astype(f32)
            mean_square = jnp.mean(attended * attended, axis=1, keepdims=True)
            gated = attended * lax.rsqrt(mean_square + 1e-06) * gates.astype(f32)
            gout[j, :, :, columns] = gated.astype(bf16).reshape(nh, 2 * cap, head_size)
        for d in farthest_first:
            give(j, d).start()

    def stage(j, carry):
        @pl.when(j < steps)
        def _():
            mine = emb.at[j, x]
            with jax.named_scope("row_wait"):
                pltpu.make_async_copy(mine, mine, row_recv.at[j]).wait()
            for d in farthest_first:
                forward(j, d).start()

        @pl.when(j >= LAG)
        def _():
            compute(j - LAG)

        return carry

    lax.fori_loop(0, steps + LAG, stage, 0)

    for d in range(1, nh):
        piece = wfull.at[(x + nh - d) % nh, 1 - c]
        with jax.named_scope("wp_wait"):
            pltpu.make_async_copy(piece, piece, wp_recv.at[d - 1]).wait()

    def collect(j, carry):
        for d in range(1, nh):
            theirs = gat.at[j, (x + nh - d) % nh]
            with jax.named_scope("gat_wait"):
                pltpu.make_async_copy(theirs, theirs, gat_recv.at[j, d - 1]).wait()
        gat[j, x] = gout[j, x]
        return carry

    def scored(first, count):
        own, width = count * 2 * cap, gat.shape[-1]
        summed = jnp.zeros((own, d_model), f32)
        for y in range(nh):
            summed = summed + jnp.dot(
                gat[first : first + count, y].reshape(own, width),
                wfull[y].reshape(width, d_model),
                preferred_element_type=f32,
            )
        mine = emb[first : first + count, pl.ds(x, 1)].reshape(own, d_model).astype(f32)
        inner = jnp.sum(summed * mine, axis=1, keepdims=True)
        square = jnp.sum(summed * summed, axis=1, keepdims=True)
        score = inner * d_model ** (-0.5) * lax.rsqrt(square / d_model + 1e-06)
        row = lax.broadcasted_iota(i32, (own, n), 0)
        slot = ((first + (row >> log2(2 * cap))) * nh + x) * (2 * cap) + (row & (2 * cap - 1))
        return jnp.sum(jnp.where(slot == slots[...], score, 0.0), axis=0, keepdims=True)

    lax.fori_loop(0, steps - 1, collect, 0)
    part[...] = scored(0, steps - 1)
    collect(steps - 1, 0)
    part[...] += scored(steps - 1, 1)

    def share(d):
        return to_head(part, out_ref.at[x], s_send.at[d - 1], s_recv.at[d - 1], d)

    for d in farthest_first:
        share(d).start()
    keep = pltpu.make_async_copy(part, out_ref.at[x], load_sem.at[0])
    keep.start()

    def drain(j, carry):
        for core in (0, 1):
            for make in (request, answer):
                copy, _, _, user = make(j, core)

                @pl.when(user != u)
                def _():
                    copy.wait_send()

        for d in range(1, nh):
            forward(j, d).wait_send()
            give(j, d).wait_send()
        return carry

    with jax.named_scope("drain"):
        lax.fori_loop(0, steps, drain, 0)
    for d in range(1, nh):
        half_out(d).wait_send()
        half_on(d).wait_send()
    keep.wait()
    for d in range(1, nh):
        share(d).wait_send()
        theirs = out_ref.at[(x + nh - d) % nh]
        with jax.named_scope("s_wait"):
            pltpu.make_async_copy(theirs, theirs, s_recv.at[d - 1]).wait()


def body(nz, nh, cand_ids, prefix_len, key_cache, value_cache, item_table, w_qkvu, w_out):
    n = cand_ids.shape[1]
    prefix, width = key_cache.shape[1:]
    shard_rows, d_model = item_table.shape
    steps = nz // nh
    blocks = 2 * nz
    cap = 2 * n // blocks
    bf16, dma = jnp.bfloat16, pltpu.SemaphoreType.DMA
    hbm = pl.BlockSpec(memory_space=pl.ANY)
    wq_width = w_qkvu.size // d_model
    parts = pl.pallas_call(
        functools.partial(kernel, nz, nh, cap),
        out_shape=jax.ShapeDtypeStruct((nh, 1, n), jnp.float32),
        in_specs=[hbm] * 7,
        out_specs=hbm,
        scratch_shapes=[
            pltpu.VMEM((1, n), jnp.int32),
            pltpu.SMEM((1,), jnp.int32),
            pltpu.VMEM((shard_rows, d_model), bf16),
            pltpu.VMEM(w_qkvu.shape, bf16),
            pltpu.VMEM((d_model, wq_width), bf16),
            pltpu.VMEM((prefix, width), bf16),
            pltpu.VMEM((prefix, width), bf16),
            pltpu.VMEM((nh, *w_out.shape), bf16),
            pltpu.VMEM((blocks, 1, 128), jnp.int32),
            pltpu.VMEM((steps, 2, 1, 128), jnp.int32),
            pltpu.VMEM((steps, 2, cap, d_model), bf16),
            pltpu.VMEM((steps, nh, 2, cap, d_model), bf16),
            pltpu.VMEM((steps, nh, 2 * cap, width), bf16),
            pltpu.VMEM((steps, nh, 2 * cap, width), bf16),
            pltpu.VMEM((1, n), jnp.int32),
            pltpu.VMEM((1, n), jnp.float32),
            dma((7,)),
            dma((steps, 2)),
            dma((steps,)),
            dma((steps, 2)),
            dma((steps,)),
            dma((steps, nh - 1)),
            dma((steps, nh - 1)),
            dma((steps, nh - 1)),
            dma((steps, nh - 1)),
            dma((nh - 1,)),
            dma((nh - 1,)),
            dma((nh - 1,)),
            dma((nh - 1,)),
            dma((nh - 1,)),
            dma((nh - 1,)),
        ],
        compiler_params=pltpu.CompilerParams(
            collective_id=0, has_side_effects=True, vmem_limit_bytes=67_043_328
        ),
    )(cand_ids, prefix_len, key_cache, value_cache, item_table, w_qkvu, w_out)
    return jnp.sum(parts, axis=0)


def solution(mesh):
    users = ("grp", "user")
    return jax.shard_map(
        functools.partial(body, mesh.shape["user"] // 2, mesh.shape["head"]),
        mesh=mesh,
        in_specs=(
            P(users, None),
            P(users),
            P(users, None, "head"),
            P(users, None, "head"),
            P("user", None),
            P(None, "head", None, None),
            P("head", None, None),
        ),
        out_specs=P(users, None),
        check_vma=False,
    )
```

```python
import functools

import jax
import jax.numpy as jnp
from jax import lax
from jax.experimental import pallas as pl
from jax.experimental.pallas import tpu as pltpu
from jax.sharding import PartitionSpec as P

MESH = pl.DeviceIdType.MESH
LAG = 2
NT = (((1,), (1,)), ((), ()))
TN = (((0,), (0,)), ((), ()))


def log2(n):
    assert n & (n - 1) == 0
    return n.bit_length() - 1


def silu(v):
    half = 0.5 * v
    return half + half * jnp.tanh(half)


def kernel(
    nz, nh, cap, ids_hbm, len_hbm, k_hbm, v_hbm, table_hbm, wq_hbm, wo_hbm, out_ref,
    ids_ref, len_ref, table, wq_in, wq, keys, values, wfull, req, req_in, rows, emb, gout, gat, slots, part,
    load_sem, req_send, req_recv, row_send, row_recv, fwd_send, fwd_recv, gat_send, gat_recv,
    w_send, w_recv, wp_send, wp_recv, s_send, s_recv,
):
    f32, bf16, i32 = jnp.float32, jnp.bfloat16, jnp.int32
    u, x = lax.axis_index("user"), lax.axis_index("head")
    z, c = u // 2, u % 2
    steps = nz // nh
    n = ids_hbm.shape[1]
    shard_rows, d_model = table.shape
    blocks = 2 * nh * steps
    own_class = (x + c * (nh // 2)) % nh

    def offset(quarter, j):
        flip = quarter // (nh // 2 + 1)
        half, back = j // 2, (j + flip) % 2
        return quarter + nh * (half + back * (steps - 1 - 2 * half))

    def shard(j, core):
        quarter = (x + core * (nh // 2)) % nh
        return 2 * ((z + offset(quarter, j)) % nz) + core

    def requester(j, core):
        return 2 * ((z + nz - offset(own_class, j)) % nz) + core

    def head(d):
        return (x + d) % nh

    partner = u + 1 - 2 * c
    farthest_first = sorted(range(1, nh), key=lambda d: -min(d, nh - d))

    barrier = pltpu.get_barrier_semaphore()

    def greet(j, carry):
        for core in (0, 1):
            for user in (shard(j, core), requester(j, core)):

                @pl.when(user != u)
                def _():
                    pl.semaphore_signal(
                        barrier, inc=1, device_id={"user": user}, device_id_type=MESH
                    )

        return carry

    lax.fori_loop(0, steps, greet, 0)
    for d in range(1, nh):
        pl.semaphore_signal(barrier, inc=1, device_id={"head": head(d)}, device_id_type=MESH)
    pl.semaphore_signal(barrier, inc=1, device_id={"user": partner}, device_id_type=MESH)

    loads = [
        pltpu.make_async_copy(src, dst, load_sem.at[i])
        for i, (src, dst) in enumerate(
            (
                (table_hbm, table),
                (wq_hbm, wq_in),
                (k_hbm.at[0], keys),
                (v_hbm.at[0], values),
                (wo_hbm, wfull.at[x]),
                (ids_hbm, ids_ref),
                (len_hbm, len_ref),
            )
        )
    ]
    for load in loads[5:] + loads[:5]:
        load.start()
    loads[5].wait()

    ids = ids_ref[...]
    shard_of = ids >> log2(shard_rows)
    local = ids & (shard_rows - 1)
    core_of = shard_of & 1
    off = ((shard_of >> 1) - z) & (nz - 1)
    turn = off >> log2(nh)
    quarter_of = off & (nh - 1)
    owner = (quarter_of - core_of * (nh // 2)) & (nh - 1)
    flip_of = jnp.where(quarter_of > nh // 2, 1, 0)
    step_of = jnp.where(
        turn < steps // 2, 2 * turn + flip_of, 2 * (steps - 1 - turn) + 1 - flip_of
    )
    block_of = (step_of * nh + owner) * 2 + core_of
    in_block = lax.broadcasted_iota(i32, (blocks, n), 0) == block_of
    one_hot = jnp.where(in_block, 1.0, 0.0).astype(bf16)
    before = lax.broadcasted_iota(i32, (n, n), 0) < lax.broadcasted_iota(i32, (n, n), 1)
    earlier = jnp.dot(
        one_hot, jnp.where(before, 1.0, 0.0).astype(bf16), preferred_element_type=f32
    )
    place = jnp.sum(jnp.where(in_block, earlier, 0.0), axis=0, keepdims=True).astype(i32)
    slots[...] = block_of * cap + place
    at_place = (lax.broadcasted_iota(i32, (128, n), 0) & (cap - 1)) == place
    high = jnp.where(at_place, (local >> 5).astype(f32), 0.0).astype(bf16)
    low = jnp.where(at_place, (local & 31).astype(f32), 0.0).astype(bf16)
    wanted = (
        lax.dot_general(one_hot, high, NT, preferred_element_type=f32) * 32.0
        + lax.dot_general(one_hot, low, NT, preferred_element_type=f32)
    ).astype(i32)
    for b in range(blocks):
        req[b] = wanted[b : b + 1]

    others = (own_class + nh - 1) // nh
    with jax.named_scope("barrier"):
        pl.semaphore_wait(barrier, 4 * steps + nh - 2 + 2 * others)

    def to_user(src, dst, send_sem, recv_sem, user):
        return pltpu.make_async_remote_copy(
            src_ref=src,
            dst_ref=dst,
            send_sem=send_sem,
            recv_sem=recv_sem,
            device_id={"user": user},
            device_id_type=MESH,
        )

    def to_head(src, dst, send_sem, recv_sem, d):
        return pltpu.make_async_remote_copy(
            src_ref=src,
            dst_ref=dst,
            send_sem=send_sem,
            recv_sem=recv_sem,
            device_id={"head": head(d)},
            device_id_type=MESH,
        )

    def start_unless_self(copy, src, dst, recv_sem, user):
        @pl.when(user != u)
        def _():
            copy.start()

        @pl.when(user == u)
        def _():
            pltpu.make_async_copy(src, dst, recv_sem).start()

    def request(j, core):
        user = shard(j, core)
        src, dst = req.at[(j * nh + x) * 2 + core], req_in.at[j, c]
        return to_user(src, dst, req_send.at[j, core], req_recv.at[j], user), src, dst, user

    def ask(j, carry):
        for core in (0, 1):
            copy, src, dst, user = request(j, core)
            start_unless_self(copy, src, dst, req_recv.at[j], user)
        return carry

    with jax.named_scope("ask"):
        lax.fori_loop(0, steps, ask, 0)

    def half_out(d):
        return to_head(wo_hbm.at[c], wfull.at[x, c], w_send.at[d - 1], w_recv.at[d - 1], d)

    loads[0].wait()

    def answer(j, core):
        user = requester(j, core)
        src, dst = rows.at[j, core], emb.at[j, x, c]
        return to_user(src, dst, row_send.at[j, core], row_recv.at[j], user), src, dst, user

    def serve(j, carry):
        with jax.named_scope("req_wait"):
            pltpu.make_async_copy(req_in.at[j], req_in.at[j], req_recv.at[j]).wait()
        lane = lax.broadcasted_iota(i32, (1, 2 * cap), 1)
        both = jnp.where(lane < cap, req_in[j, 0][:, : 2 * cap], req_in[j, 1][:, : 2 * cap])
        pick = lax.broadcasted_iota(i32, (shard_rows, 2 * cap), 0) == both
        found = lax.dot_general(
            jnp.where(pick, 1.0, 0.0).astype(bf16), table[...], TN, preferred_element_type=f32
        )
        rows[j] = found.astype(bf16).reshape(2, cap, d_model)
        for core in (0, 1):
            copy, src, dst, user = answer(j, core)
            start_unless_self(copy, src, dst, row_recv.at[j], user)
        return carry

    lax.fori_loop(0, steps, serve, 0)
    for d in range(1, nh):
        half_out(d).start()

    def half_on(d):
        piece = wfull.at[(x + nh - d) % nh, c]
        return to_user(piece, piece, wp_send.at[d - 1], wp_recv.at[d - 1], partner)

    for load in loads[1:5] + loads[6:]:
        load.wait()
    span = 128

    def relay_weights(i, carry):
        at = pl.ds(pl.multiple_of(i * span, span), span)
        wq[at, :] = wq_in[at].reshape(span, wq.shape[1])
        return carry

    with jax.named_scope("relay"):
        lax.fori_loop(0, d_model // span, relay_weights, 0)

    length = len_ref[0]
    head_size = 128
    heads_here = keys.shape[1] // head_size
    prefix = keys.shape[0]
    scale = head_size ** (-0.5)
    per_token = 1.0 / (jnp.zeros((1, 1), f32) + (length + 1).astype(f32))
    inside = lax.broadcasted_iota(i32, (1, prefix), 1) < length
    factor = jnp.where(inside, (0.5 * scale) * per_token, 0.0)

    def forward(j, d):
        mine = emb.at[j, x]
        return to_head(mine, mine, fwd_send.at[j, d - 1], fwd_recv.at[j, d - 1], d)

    def give(j, d):
        return to_head(
            gout.at[j, head(d)], gat.at[j, x], gat_send.at[j, d - 1], gat_recv.at[j, d - 1], d
        )

    def compute(j):
        for d in range(1, nh):
            theirs = emb.at[j, (x + nh - d) % nh]
            with jax.named_scope("fwd_wait"):
                pltpu.make_async_copy(theirs, theirs, fwd_recv.at[j, d - 1]).wait()
        embedded = emb[j].reshape(nh * 2 * cap, d_model)
        projected = jnp.dot(embedded, wq[...], preferred_element_type=f32)
        activated = silu(projected).astype(bf16)
        for h in range(heads_here):
            columns = slice(h * head_size, (h + 1) * head_size)
            queries, own_keys, own_values, gates = (
                activated[:, (4 * h + i) * head_size : (4 * h + i + 1) * head_size]
                for i in range(4)
            )
            raw = lax.dot_general(queries, keys[:, columns], NT, preferred_element_type=f32)
            weights = (raw * factor) * (1.0 + jnp.tanh(raw * (0.5 * scale)))
            attended = jnp.dot(
                weights.astype(bf16), values[:, columns], preferred_element_type=f32
            )
            own_dot = jnp.sum(
                queries.astype(f32) * own_keys.astype(f32), axis=1, keepdims=True
            )
            own_weight = silu(own_dot * scale) * per_token
            attended = attended + own_weight * own_values.astype(f32)
            mean_square = jnp.mean(attended * attended, axis=1, keepdims=True)
            gated = attended * lax.rsqrt(mean_square + 1e-06) * gates.astype(f32)
            gout[j, :, :, columns] = gated.astype(bf16).reshape(nh, 2 * cap, head_size)
        for d in farthest_first:
            give(j, d).start()

    def stage(j, carry):
        @pl.when(j < steps)
        def _():
            mine = emb.at[j, x]
            with jax.named_scope("row_wait"):
                pltpu.make_async_copy(mine, mine, row_recv.at[j]).wait()
            for d in farthest_first:
                forward(j, d).start()

        @pl.when(j == steps // 2)
        def _():
            for d in range(1, nh):
                piece = wfull.at[(x + nh - d) % nh, c]
                with jax.named_scope("w_wait"):
                    pltpu.make_async_copy(piece, piece, w_recv.at[d - 1]).wait()
                half_on(d).start()

        @pl.when(j >= LAG)
        def _():
            compute(j - LAG)

        return carry

    lax.fori_loop(0, steps + LAG, stage, 0)

    for d in range(1, nh):
        piece = wfull.at[(x + nh - d) % nh, 1 - c]
        with jax.named_scope("wp_wait"):
            pltpu.make_async_copy(piece, piece, wp_recv.at[d - 1]).wait()

    def collect(j, carry):
        for d in range(1, nh):
            theirs = gat.at[j, (x + nh - d) % nh]
            with jax.named_scope("gat_wait"):
                pltpu.make_async_copy(theirs, theirs, gat_recv.at[j, d - 1]).wait()
        gat[j, x] = gout[j, x]
        return carry

    def scored(first, count):
        own, width = count * 2 * cap, gat.shape[-1]
        summed = jnp.zeros((own, d_model), f32)
        for y in range(nh):
            summed = summed + jnp.dot(
                gat[first : first + count, y].reshape(own, width),
                wfull[y].reshape(width, d_model),
                preferred_element_type=f32,
            )
        mine = emb[first : first + count, pl.ds(x, 1)].reshape(own, d_model).astype(f32)
        inner = jnp.sum(summed * mine, axis=1, keepdims=True)
        square = jnp.sum(summed * summed, axis=1, keepdims=True)
        score = inner * d_model ** (-0.5) * lax.rsqrt(square / d_model + 1e-06)
        row = lax.broadcasted_iota(i32, (own, n), 0)
        slot = ((first + (row >> log2(2 * cap))) * nh + x) * (2 * cap) + (row & (2 * cap - 1))
        return jnp.sum(jnp.where(slot == slots[...], score, 0.0), axis=0, keepdims=True)

    lax.fori_loop(0, steps - 1, collect, 0)
    part[...] = scored(0, steps - 1)
    collect(steps - 1, 0)
    part[...] += scored(steps - 1, 1)

    def share(d):
        return to_head(part, out_ref.at[x], s_send.at[d - 1], s_recv.at[d - 1], d)

    for d in farthest_first:
        share(d).start()
    keep = pltpu.make_async_copy(part, out_ref.at[x], load_sem.at[0])
    keep.start()

    def drain(j, carry):
        for core in (0, 1):
            for make in (request, answer):
                copy, _, _, user = make(j, core)

                @pl.when(user != u)
                def _():
                    copy.wait_send()

        for d in range(1, nh):
            forward(j, d).wait_send()
            give(j, d).wait_send()
        return carry

    with jax.named_scope("drain"):
        lax.fori_loop(0, steps, drain, 0)
    for d in range(1, nh):
        half_out(d).wait_send()
        half_on(d).wait_send()
    keep.wait()
    for d in range(1, nh):
        share(d).wait_send()
        theirs = out_ref.at[(x + nh - d) % nh]
        with jax.named_scope("s_wait"):
            pltpu.make_async_copy(theirs, theirs, s_recv.at[d - 1]).wait()


def body(nz, nh, cand_ids, prefix_len, key_cache, value_cache, item_table, w_qkvu, w_out):
    n = cand_ids.shape[1]
    prefix, width = key_cache.shape[1:]
    shard_rows, d_model = item_table.shape
    steps = nz // nh
    blocks = 2 * nz
    cap = 2 * n // blocks
    bf16, dma = jnp.bfloat16, pltpu.SemaphoreType.DMA
    hbm = pl.BlockSpec(memory_space=pl.ANY)
    wq_width = w_qkvu.size // d_model
    parts = pl.pallas_call(
        functools.partial(kernel, nz, nh, cap),
        out_shape=jax.ShapeDtypeStruct((nh, 1, n), jnp.float32),
        in_specs=[hbm] * 7,
        out_specs=hbm,
        scratch_shapes=[
            pltpu.VMEM((1, n), jnp.int32),
            pltpu.SMEM((1,), jnp.int32),
            pltpu.VMEM((shard_rows, d_model), bf16),
            pltpu.VMEM(w_qkvu.shape, bf16),
            pltpu.VMEM((d_model, wq_width), bf16),
            pltpu.VMEM((prefix, width), bf16),
            pltpu.VMEM((prefix, width), bf16),
            pltpu.VMEM((nh, *w_out.shape), bf16),
            pltpu.VMEM((blocks, 1, 128), jnp.int32),
            pltpu.VMEM((steps, 2, 1, 128), jnp.int32),
            pltpu.VMEM((steps, 2, cap, d_model), bf16),
            pltpu.VMEM((steps, nh, 2, cap, d_model), bf16),
            pltpu.VMEM((steps, nh, 2 * cap, width), bf16),
            pltpu.VMEM((steps, nh, 2 * cap, width), bf16),
            pltpu.VMEM((1, n), jnp.int32),
            pltpu.VMEM((1, n), jnp.float32),
            dma((7,)),
            dma((steps, 2)),
            dma((steps,)),
            dma((steps, 2)),
            dma((steps,)),
            dma((steps, nh - 1)),
            dma((steps, nh - 1)),
            dma((steps, nh - 1)),
            dma((steps, nh - 1)),
            dma((nh - 1,)),
            dma((nh - 1,)),
            dma((nh - 1,)),
            dma((nh - 1,)),
            dma((nh - 1,)),
            dma((nh - 1,)),
        ],
        compiler_params=pltpu.CompilerParams(
            collective_id=0, has_side_effects=True, vmem_limit_bytes=67_043_328
        ),
    )(cand_ids, prefix_len, key_cache, value_cache, item_table, w_qkvu, w_out)
    return jnp.sum(parts, axis=0)


def solution(mesh):
    users = ("grp", "user")
    return jax.shard_map(
        functools.partial(body, mesh.shape["user"] // 2, mesh.shape["head"]),
        mesh=mesh,
        in_specs=(
            P(users, None),
            P(users),
            P(users, None, "head"),
            P(users, None, "head"),
            P("user", None),
            P(None, "head", None, None),
            P("head", None, None),
        ),
        out_specs=P(users, None),
        check_vma=False,
    )
```
